256 devices in a mesh: seq: 128 (over y_hi, x, z, core), grp: 2 (over y_lo).
Axes of the slice: x: 4, y: 4 (y_hi: 2, y_lo: 2; y = y_hi * 2 + y_lo), z: 8, core: 2. Of those that a mesh axis runs over, the one named last changes fastest.
Arguments:
- prefill_queries: bfloat16 [8192, 4096], P('seq', 'grp'), may hold values from -6 to 6
- prefill_keys: bfloat16 [8192, 512], P('seq', 'grp'), may hold values from -6 to 6
- prefill_values: bfloat16 [8192, 512], P('seq', 'grp'), may hold values from -6 to 6
- block_mask: int32 [128, 128], replicated, may hold values 0 or 1
- bit_widths: int32 [4], P('grp'), may hold values from 3 to 8
- scale_exps: int32 [4], P('grp'), may hold values from 1 to 4
- decode_queries: bfloat16 [4, 256, 4096], P(None, 'seq', 'grp'), may hold values from -6 to 6
- new_keys: bfloat16 [4, 256, 512], P(None, 'seq', 'grp'), may hold values from -6 to 6
- new_values: bfloat16 [4, 256, 512], P(None, 'seq', 'grp'), may hold values from -6 to 6
- context_len: int32 [256], P('seq'), may hold values from 1 to 8192
Outputs:
- prefill_out: bfloat16 [8192, 4096], P('seq', 'grp')
- decode_out: bfloat16 [4, 256, 4096], P(None, 'seq', 'grp')
The draws below stay inside these ranges and needn't reach their ends.
All inputs are finite; a program needn't handle non-finite values.
Results may differ from the reference program's by a relative error of at most 0.012.
Values may be sent and summed in bfloat16 or wider, within the bound.
A program may use at most 64 MiB of HBM per device.

```python
import math
import jax
import jax.numpy as jnp
from jax import lax

HEADS = 32
KV_HEADS = 4
HEAD = 128
TOK_DEV = 64
ROW_DEV = 2
STEPS = 4
TOKENS = 8192
ROWS = 256
BLOCKS = 128


def prefill_pair(key):
    query_seed, key_seed = jax.random.split(key, 2)
    queries = jnp.clip(jax.random.normal(query_seed, (TOKENS, HEADS * HEAD), jnp.float32), -6.0, 6.0)
    keys_drawn = jnp.clip(jax.random.normal(key_seed, (TOKENS, KV_HEADS * HEAD), jnp.float32), -6.0, 6.0)
    return (queries, keys_drawn)


def decode_pair(key):
    query_seed, key_seed = jax.random.split(key, 2)
    queries = jnp.clip(jax.random.normal(query_seed, (STEPS, ROWS, HEADS * HEAD), jnp.float32), -6.0, 6.0)
    keys_drawn = jnp.clip(jax.random.normal(key_seed, (STEPS, ROWS, KV_HEADS * HEAD), jnp.float32), -6.0, 6.0)
    return (queries, keys_drawn)


def draw_prefill_queries(key, part):
    return prefill_pair(jax.random.fold_in(key, 11))[0].astype(jnp.bfloat16)


def draw_prefill_keys(key, part):
    return prefill_pair(jax.random.fold_in(key, 11))[1].astype(jnp.bfloat16)


def draw_decode_queries(key, part):
    return decode_pair(jax.random.fold_in(key, 23))[0].astype(jnp.bfloat16)


def draw_new_keys(key, part):
    return decode_pair(jax.random.fold_in(key, 23))[1].astype(jnp.bfloat16)


def place_ends(result, rng, smallest, largest):
    longest = result.shape.index(max(result.shape))
    spots = []
    for shift in (0, 1):
        where = [jax.random.randint(jax.random.fold_in(rng, axis), (), 0, length) for axis, length in enumerate(result.shape)]
        where[longest] = (where[longest] + shift) % result.shape[longest]
        spots.append(tuple(where))
    return result.at[spots[0]].set(smallest).at[spots[1]].set(largest)


def block_levels(rng, extent, cuts, smallest, top_value):
    loudness = 1.0
    for position, blocks in cuts:
        draws = jax.random.uniform(jax.random.fold_in(jax.random.fold_in(rng, 6), position), (blocks,), jnp.float32, smallest / len(cuts), top_value / len(cuts))
        loudness = loudness * jnp.repeat(jnp.exp(draws), extent[position] // blocks).reshape((-1,) + (1,) * (len(extent) - 1 - position))
    return loudness


def centred(own_key, shape, spread, limit, cuts=(), kind=jnp.bfloat16):
    values = jax.random.normal(own_key, shape, jnp.float32) * spread
    if len(cuts) > 0:
        values = block_levels(own_key, shape, cuts, -0.22, 0.18) * values
    return jnp.clip(values, min=-limit, max=limit).astype(kind)


def setup_inputs(seed: int = 0) -> dict:
    arg_keys = jax.random.split(jax.random.key(seed), 11)
    return {
        "prefill_queries": draw_prefill_queries(jax.random.fold_in(arg_keys[10], 71), 0),
        "prefill_keys": draw_prefill_keys(jax.random.fold_in(arg_keys[10], 71), 0),
        "prefill_values": centred(arg_keys[2], (TOKENS, KV_HEADS * HEAD), 1.0, 6.0, ((0, 128), (1, 2))),
        "block_mask": place_ends((jax.random.randint(arg_keys[3], (BLOCKS, BLOCKS), 0, 2) < 1).astype(jnp.int32), jax.random.fold_in(arg_keys[3], 1), 0, 1),
        "bit_widths": place_ends(jax.random.randint(arg_keys[4], (KV_HEADS,), 3, 9), jax.random.fold_in(arg_keys[4], 1), 3, 8).astype(jnp.int32),
        "scale_exps": place_ends(jax.random.randint(arg_keys[5], (KV_HEADS,), 1, 5), jax.random.fold_in(arg_keys[5], 1), 1, 4).astype(jnp.int32),
        "decode_queries": draw_decode_queries(jax.random.fold_in(arg_keys[10], 71), 0),
        "new_keys": draw_new_keys(jax.random.fold_in(arg_keys[10], 71), 0),
        "new_values": centred(arg_keys[8], (STEPS, ROWS, KV_HEADS * HEAD), 1.0, 6.0, ((1, 128), (2, 2))),
        "context_len": place_ends(jax.random.randint(arg_keys[9], (ROWS,), 1, TOKENS + 1), jax.random.fold_in(arg_keys[9], 1), 1, TOKENS).astype(jnp.int32),
    }


very_low = -1e+30
norm_eps = 1e-06

def sign_table(order):
    positions = jnp.arange(order, dtype=jnp.int32)
    common_bits = positions[:, None] & positions[None, :]
    parity = jnp.zeros((order, order), jnp.int32)
    for bit_number in range(order.bit_length() - 1):
        parity = parity + (common_bits >> bit_number & 1)
    return (1 - 2 * (parity % 2)).astype(jnp.float32)

def level_terms(bit_widths, scale_exps):
    clip_level = 2.0 ** (bit_widths.astype(jnp.float32) - 1.0) - 1.0
    forward = 2.0 ** scale_exps.astype(jnp.float32) / math.sqrt(HEAD)
    backward = 2.0 ** (-scale_exps.astype(jnp.float32)) / math.sqrt(HEAD)
    return (clip_level, forward, backward)

def encode_rows(shaped, sign_matrix, clip_level, forward):
    rotated = jnp.dot(shaped, sign_matrix, preferred_element_type=jnp.float32)
    levels = jnp.floor(rotated * forward[:, None] + 0.5)
    limited = jnp.clip(levels, -clip_level[:, None], clip_level[:, None])
    return limited.astype(jnp.bfloat16)

def decode_rows(encoded, sign_matrix, backward):
    restored = jnp.dot(encoded, sign_matrix, preferred_element_type=jnp.float32)
    return (restored * backward[:, None]).astype(jnp.bfloat16)

def rounded(weights):
    return lax.optimization_barrier(weights.astype(jnp.bfloat16)).astype(jnp.float32)

def head_norm(attn):
    mean_square = lax.optimization_barrier(jnp.sum(attn * attn, axis=-1, keepdims=True)) / (HEADS * HEAD)
    return (attn * lax.rsqrt(mean_square + norm_eps)).astype(jnp.bfloat16)

def reference(prefill_queries, prefill_keys, prefill_values, block_mask, bit_widths, scale_exps, decode_queries, new_keys, new_values, context_len):
    group_size = HEADS // KV_HEADS
    score_scale = 1.0 / math.sqrt(HEAD)
    sign_matrix = sign_table(HEAD).astype(jnp.bfloat16)
    clip_level, forward, backward = level_terms(bit_widths, scale_exps)
    key_rows = prefill_keys.reshape(TOKENS, KV_HEADS, HEAD)
    value_rows = prefill_values.reshape(TOKENS, KV_HEADS, HEAD)
    keys_wide = key_rows.astype(jnp.float32)
    values_wide = value_rows.astype(jnp.float32)
    key_pos = jnp.arange(TOKENS, dtype=jnp.int32)
    key_block = key_pos // TOK_DEV

    def prefill_block(block_index):
        queries = lax.dynamic_slice_in_dim(prefill_queries, block_index * TOK_DEV, TOK_DEV, 0)
        queries = queries.reshape(TOK_DEV, KV_HEADS, group_size, HEAD).astype(jnp.float32)
        query_pos = block_index * TOK_DEV + jnp.arange(TOK_DEV, dtype=jnp.int32)
        mask_row = block_mask[block_index]
        block_open = (key_block == block_index) | (mask_row[key_block] == 1)
        allowed = ((key_pos[None, :] <= query_pos[:, None]) & block_open[None, :])[:, None, None, :]
        scores = jnp.einsum('tkgd,skd->tkgs', queries, keys_wide) * score_scale
        masked = jnp.where(allowed, scores, very_low)
        top = lax.optimization_barrier(jnp.max(masked, axis=-1, keepdims=True))
        weights = jnp.where(allowed, jnp.exp(masked - top), 0.0)
        weight_sum = lax.optimization_barrier(jnp.sum(weights, axis=-1))
        mixed = jnp.einsum('tkgs,skd->tkgd', rounded(weights), values_wide)
        return (mixed / weight_sum[..., None]).reshape(TOK_DEV, HEADS * HEAD)
    prefill_attn = lax.map(prefill_block, jnp.arange(BLOCKS, dtype=jnp.int32)).reshape(TOKENS, HEADS * HEAD)
    cache_keys = decode_rows(encode_rows(key_rows, sign_matrix, clip_level, forward), sign_matrix, backward).astype(jnp.float32)
    cache_values = decode_rows(encode_rows(value_rows, sign_matrix, clip_level, forward), sign_matrix, backward).astype(jnp.float32)
    all_queries = decode_queries.reshape(STEPS, ROWS, KV_HEADS, group_size, HEAD).astype(jnp.float32)
    own_keys = new_keys.reshape(STEPS, ROWS, KV_HEADS, HEAD).astype(jnp.float32)
    own_values = new_values.reshape(STEPS, ROWS, KV_HEADS, HEAD).astype(jnp.float32)
    step_pos = jnp.arange(STEPS, dtype=jnp.int32)
    own_allowed = (step_pos[None, :] <= step_pos[:, None])[:, None, None, None, :]

    def decode_block(block_index):
        queries = lax.dynamic_slice_in_dim(all_queries, block_index * ROW_DEV, ROW_DEV, 1)
        block_keys = lax.dynamic_slice_in_dim(own_keys, block_index * ROW_DEV, ROW_DEV, 1)
        block_values = lax.dynamic_slice_in_dim(own_values, block_index * ROW_DEV, ROW_DEV, 1)
        limits = lax.dynamic_slice_in_dim(context_len, block_index * ROW_DEV, ROW_DEV, 0)
        cache_open = (key_pos[None, :] < limits[:, None])[None, :, None, None, :]
        cache_scores = jnp.einsum('trkgd,pkd->trkgp', queries, cache_keys) * score_scale
        own_scores = jnp.einsum('trkgd,urkd->trkgu', queries, block_keys) * score_scale
        cache_masked = jnp.where(cache_open, cache_scores, very_low)
        own_masked = jnp.where(own_allowed, own_scores, very_low)
        top = jnp.maximum(lax.optimization_barrier(jnp.max(cache_masked, axis=-1)), lax.optimization_barrier(jnp.max(own_masked, axis=-1)))[..., None]
        cache_weights = jnp.where(cache_open, jnp.exp(cache_masked - top), 0.0)
        own_weights = jnp.where(own_allowed, jnp.exp(own_masked - top), 0.0)
        weight_sum = lax.optimization_barrier(jnp.sum(cache_weights, axis=-1)) + lax.optimization_barrier(jnp.sum(own_weights, axis=-1))
        mixed = jnp.einsum('trkgp,pkd->trkgd', rounded(cache_weights), cache_values)
        mixed = mixed + jnp.einsum('trkgu,urkd->trkgd', rounded(own_weights), block_values)
        return (mixed / weight_sum[..., None]).reshape(STEPS, ROW_DEV, HEADS * HEAD)
    stacked = lax.map(decode_block, jnp.arange(BLOCKS, dtype=jnp.int32))
    decode_attn = jnp.moveaxis(stacked, 0, 1).reshape(STEPS, ROWS, HEADS * HEAD)
    return (head_norm(prefill_attn), head_norm(decode_attn))
```

```python
import math

import jax
import jax.numpy as jnp
import numpy as np
from jax import lax
from jax.experimental import pallas as pl
from jax.experimental.pallas import tpu as pltpu
from jax.sharding import PartitionSpec as P

HEADS = 32
KV = 2
GROUP = 8
HEAD = 128
STEPS = 4
TOK = 64
ROWS = 2
XS, ZS = 4, 8
HALF = TOK // 2
UNIT = 2 * HALF
TILE = 512
VERY_LOW = -1e30
EPS = 1e-6
WIDE = HEADS * HEAD
SCORE = math.log2(math.e) / math.sqrt(HEAD)

BF = jnp.bfloat16
F32 = jnp.float32
MESH = pl.DeviceIdType.MESH

OFFSETS = [(dx, dz) for dx in (0, -1, 1, 2) for dz in (0, -1, 1, -2, 2, -3, 3, 4)]
WAVES = [[o for o in OFFSETS if abs(o[0]) + abs(o[1]) == d] for d in range(7)]
SLOT = {}
START = []
for wave in WAVES:
    START.append(len(SLOT) * UNIT)
    for path in (0, 1):
        for off in wave:
            SLOT[(path, *off)] = len(SLOT)
START.append(len(SLOT) * UNIT)
OWN = START[-1]
NTILE = OWN // TILE
FIRST = [max(0, (START[d] // TILE)) for d in range(7)]
TABLE = np.array(
    [path * 64 + (dx % XS) * 8 + dz % ZS for (path, dx, dz) in SLOT], np.int32
)


def x_moves(dx):
    return {
        0: [("x", 1, -1, None), ("x", -1, 1, None)],
        -1: [("x", 1, 2, 0)],
        1: [("x", -1, 2, 1)],
        2: [],
    }[dx]


def z_moves(dz):
    if dz == 0:
        return [("z", 1, -1, None), ("z", -1, 1, None)]
    if dz == 4:
        return []
    way = 1 if dz < 0 else -1
    if abs(dz) == 3:
        return [("z", way, 4, 0 if dz < 0 else 1)]
    return [("z", way, dz - way, None)]


def moves(path, dx, dz):
    out = []
    if path == 0 or dx == 0:
        out += [(a, w, SLOT[(path, dx, n)], h) for a, w, n, h in z_moves(dz)]
    if path == 1 or dz == 0:
        out += [(a, w, SLOT[(path, n, dz)], h) for a, w, n, h in x_moves(dx)]
    return out


def dot(a, b):
    return jnp.dot(a, b, preferred_element_type=F32)


def choose(n, first, values):
    out = jnp.float32(values[0])
    for i, v in enumerate(values[1:]):
        out = jnp.where(n == first + 1 + i, jnp.float32(v), out)
    return out


def kernel(
    table,
    widths,
    exps,
    ctx,
    q_ref,
    k_hbm,
    v_hbm,
    k_own,
    v_own,
    mask_ref,
    dq_ref,
    nk_ref,
    nv_ref,
    out_ref,
    dout_ref,
    kv,
    qx,
    qd,
    h2,
    oh,
    pos,
    m_p,
    l_p,
    o_p,
    m_d,
    l_d,
    o_d,
    m_0,
    o_0,
    dq_s,
    nk_s,
    nv_s,
    attn,
    dattn,
    sq_mine,
    sq_theirs,
    load_sem,
    y_send,
    y_recv,
    send_sem,
    recv_sem,
    sib_send,
    sib_recv,
    g_send,
    g_recv,
):
    s = lax.axis_index("seq")
    grp = lax.axis_index("grp")
    core = s % 2
    z = (s // 2) % ZS
    x = (s // (2 * ZS)) % XS
    yh = s // (2 * ZS * XS)

    def at(yh_, x_, z_, core_):
        return ((yh_ * XS + x_) * ZS + z_) * 2 + core_

    peers = {
        ("x", 1): at(yh, (x + 1) % XS, z, core),
        ("x", -1): at(yh, (x + XS - 1) % XS, z, core),
        ("z", 1): at(yh, x, (z + 1) % ZS, core),
        ("z", -1): at(yh, x, (z + ZS - 1) % ZS, core),
    }
    across = at(1 - yh, x, z, core)
    sibling = at(yh, x, z, 1 - core)

    loads = []
    for path in (0, 1):
        for part, src in enumerate((k_hbm, v_hbm)):
            loads.append(
                pltpu.make_async_copy(
                    src.at[pl.ds(path * HALF, HALF), :],
                    kv.at[pl.ds(path * UNIT + yh * HALF, HALF), pl.ds(part * 256, 256)],
                    load_sem.at[path * 2 + part],
                )
            )
    for c in loads:
        c.start()

    barrier = pltpu.get_barrier_semaphore()
    for dev in (*peers.values(), across, sibling):
        pl.semaphore_signal(barrier, inc=1, device_id=(dev, grp), device_id_type=MESH)
    pl.semaphore_signal(barrier, inc=1, device_id=(s, 1 - grp), device_id_type=MESH)
    for c in loads:
        c.wait()
    pl.semaphore_wait(barrier, 7)

    def remote(src_row, dst_row, count, ssem, rsem, dev):
        return pltpu.make_async_remote_copy(
            src_ref=kv.at[pl.ds(src_row, count), :],
            dst_ref=kv.at[pl.ds(dst_row, count), :],
            send_sem=ssem,
            recv_sem=rsem,
            device_id=(dev, grp),
            device_id_type=MESH,
        )

    ycopies = []
    for path in (0, 1):
        row = path * UNIT + yh * HALF
        ycopies.append(remote(row, row, HALF, y_send.at[path], y_recv.at[path], across))
    for c in ycopies:
        c.start()

    i0 = lax.broadcasted_iota(jnp.int32, (256, 256), 0)
    i1 = lax.broadcasted_iota(jnp.int32, (256, 256), 1)
    both = (i0 & i1) & 127
    parity = jnp.zeros((256, 256), jnp.int32)
    for b in range(7):
        parity = parity + ((both >> b) & 1)
    sign = (1 - 2 * (parity % 2)).astype(F32)
    h2[...] = jnp.where((i0 // 128) == (i1 // 128), sign, 0.0).astype(BF)

    lane = lax.broadcasted_iota(jnp.int32, (1, 128), 1)
    first_head = lane < 64
    level = [choose(widths[i], 3, [3.0, 7.0, 15.0, 31.0, 63.0, 127.0]) for i in range(KV)]
    power = [choose(exps[i], 1, [2.0, 4.0, 8.0, 16.0]) for i in range(KV)]
    inverse = [choose(exps[i], 1, [0.5, 0.25, 0.125, 0.0625]) for i in range(KV)]
    forward = [p / math.sqrt(HEAD) for p in power]
    backward = [p / math.sqrt(HEAD) for p in inverse]
    limits = jnp.where(lane % 2 == 0, ctx[0], ctx[1])

    row = mask_ref[pl.ds(s, 1), :]
    closed = jnp.where((row == 1) & (lane < s), 0.0, VERY_LOW).astype(F32)
    tri = lax.broadcasted_iota(jnp.int32, (TOK, 512), 0) <= (
        lax.broadcasted_iota(jnp.int32, (TOK, 512), 1) % TOK
    )
    for kh in range(KV):
        for g in range(GROUP):
            h = kh * GROUP + g
            piece = q_ref[:, h * HEAD : (h + 1) * HEAD].astype(F32)
            cols = slice(g * TOK, (g + 1) * TOK)
            whole = jnp.concatenate([piece, jnp.broadcast_to(closed, (TOK, 128))], axis=1)
            if g % 2 == 0:
                held = whole
            else:
                two = jnp.concatenate([held, whole], axis=0)
                qx[kh, :, (g - 1) * TOK : (g + 1) * TOK] = two.T.astype(BF)
        sc = dot(k_own[:, kh * HEAD : (kh + 1) * HEAD], qx[kh, 0:128, :])
        sc = jnp.where(tri, sc, VERY_LOW)
        top = jnp.max(sc, axis=0, keepdims=True)
        w = jnp.exp2((sc - top) * SCORE)
        m_p[kh] = top
        l_p[kh] = jnp.sum(w, axis=0, keepdims=True)
        vt = v_own[:, kh * HEAD : (kh + 1) * HEAD].astype(F32).T.astype(BF)
        o_p[kh] = dot(vt, w.astype(BF))

    for h in range(KV * GROUP):
        for t in range(STEPS):
            dq_s[h * 8 + t * ROWS : h * 8 + (t + 1) * ROWS, :] = dq_ref[
                t, :, h * HEAD : (h + 1) * HEAD
            ].astype(F32)
    nk_s[...] = jnp.zeros_like(nk_s)
    nv_s[...] = jnp.zeros_like(nv_s)
    for t in range(STEPS):
        nk_s[t * ROWS : (t + 1) * ROWS, :] = nk_ref[t].astype(F32)
        nv_s[t * ROWS : (t + 1) * ROWS, :] = nv_ref[t].astype(F32)
    dq = dq_s[...]
    turned = dot(dq.astype(BF), h2[0:128, 0:128])
    which = lax.broadcasted_iota(jnp.int32, (128, 1), 0) < 64
    turned = (turned * jnp.where(which, backward[0], backward[1])).T
    high = turned.astype(BF).astype(F32)
    low = turned - high
    zero = jnp.zeros((128, 128), F32)
    for part, a in enumerate((high, low)):
        cols = slice(part * 128, (part + 1) * 128)
        qd[0:128, cols] = jnp.where(first_head, a, zero).astype(BF)
        qd[128:256, cols] = jnp.where(first_head, zero, a).astype(BF)
    dqt = dq.T
    upper = jnp.where(first_head, dqt, zero).astype(BF)
    lower = jnp.where(first_head, zero, dqt).astype(BF)
    nk = nk_s[...].astype(BF)
    sc = dot(nk[:, 0:128], upper) + dot(nk[:, 128:256], lower)
    key_i = lax.broadcasted_iota(jnp.int32, (128, 128), 0)
    qry_i = lax.broadcasted_iota(jnp.int32, (128, 128), 1) % (STEPS * ROWS)
    seen = (
        (key_i < STEPS * ROWS)
        & (key_i % ROWS == qry_i % ROWS)
        & (key_i // ROWS <= qry_i // ROWS)
    )
    sc = jnp.where(seen, sc, VERY_LOW)
    top = jnp.max(sc, axis=0, keepdims=True)
    w = jnp.where(seen, jnp.exp2((sc - top) * SCORE), 0.0)
    m_d[...] = top
    m_0[...] = top
    l_d[...] = jnp.sum(w, axis=0, keepdims=True)
    nvt = nv_s[...].T.astype(BF)
    wide = dot(nvt, w.astype(BF))
    o_0[...] = jnp.where(first_head, wide[0:128], wide[128:256])
    o_d[...] = jnp.zeros_like(o_d)

    def forwards(d):
        for path in (0, 1):
            for dx, dz in WAVES[d]:
                here = SLOT[(path, dx, dz)] * UNIT
                for axis, way, there, half in moves(path, dx, dz):
                    shift, count = (0, UNIT) if half is None else (half * HALF, HALF)
                    remote(
                        here + shift,
                        there * UNIT + shift,
                        count,
                        send_sem.at[d + 1],
                        recv_sem.at[d + 1],
                        peers[(axis, way)],
                    ).start()

    def wave_copy(d):
        return remote(
            START[d], START[d], START[d + 1] - START[d], send_sem.at[d], recv_sem.at[d], sibling
        )

    def to_sibling(d):
        return remote(
            START[d],
            OWN + START[d],
            START[d + 1] - START[d],
            sib_send.at[d],
            sib_recv.at[d],
            sibling,
        )

    for c in ycopies:
        c.wait_recv()
    forwards(0)
    to_sibling(0).start()

    def step(i, carry):
        for d in range(1, 7):
            at_step = 2 * max(FIRST[d], 0) if d > 1 else 0
            if d in (2,):
                at_step = 2 * 1

            @pl.when(i == at_step)
            def _():
                wave_copy(d).wait_recv()
                if d < 6:
                    forwards(d)
                to_sibling(d).start()

            @pl.when(i == at_step + 1)
            def _():
                if d == 1:
                    to_sibling(0).wait_recv()
                to_sibling(d).wait_recv()

        e = i % 2
        tile = i // 2
        first = pl.multiple_of(e * OWN + tile * TILE, TILE)
        rows_in = lax.broadcasted_iota(jnp.int32, (HALF, 128), 0)
        lanes_in = lax.broadcasted_iota(jnp.int32, (HALF, 128), 1)
        for u in range(TILE // UNIT):
            code = table[tile * (TILE // UNIT) + u]
            sx = (x + (code % 64) // 8) % XS
            sz = (z + code % 8) % ZS
            for y in (0, 1):
                block = at(y, sx, sz, (core + e) % 2)
                here = slice(u * UNIT + y * HALF, u * UNIT + (y + 1) * HALF)
                oh[here, :] = jnp.where(lanes_in == block, 1.0, 0.0).astype(BF)
                pos[here, :] = rows_in + (block * TOK + (code // 64) * HALF)

        keys = kv[pl.ds(first, TILE), 0:256]
        vals_t = kv[pl.ds(first, TILE), 256:512].T
        blocks = oh[...]
        for kh in range(KV):
            ext = jnp.concatenate([keys[:, kh * HEAD : (kh + 1) * HEAD], blocks], axis=1)
            sc = dot(ext, qx[kh])
            old = m_p[kh]
            top = jnp.maximum(old, jnp.max(sc, axis=0, keepdims=True))
            w = jnp.exp2(sc * SCORE - top * SCORE)
            fade = jnp.exp2((old - top) * SCORE)
            m_p[kh] = top
            l_p[kh] = l_p[kh] * fade + jnp.sum(w, axis=0, keepdims=True)
            o_p[kh] = o_p[kh] * fade + dot(vals_t[kh * HEAD : (kh + 1) * HEAD, :], w.astype(BF))

        rot = dot(keys, h2[...])
        coded = jnp.concatenate(
            [
                jnp.clip(
                    jnp.floor(rot[:, j * HEAD : (j + 1) * HEAD] * forward[j] + 0.5),
                    -level[j],
                    level[j],
                ).astype(BF)
                for j in range(KV)
            ],
            axis=1,
        )
        two = dot(coded, qd[...])
        sc = jnp.where(pos[...] < limits, two[:, 0:128] + two[:, 128:256], VERY_LOW)
        old = m_d[...]
        top = jnp.maximum(old, jnp.max(sc, axis=0, keepdims=True))
        w = jnp.exp2(sc * SCORE - top * SCORE)
        fade = jnp.exp2((old - top) * SCORE)
        m_d[...] = top
        l_d[...] = l_d[...] * fade + jnp.sum(w, axis=0, keepdims=True)
        rot = dot(h2[...], vals_t)
        coded = jnp.concatenate(
            [
                jnp.clip(
                    jnp.floor(rot[j * HEAD : (j + 1) * HEAD, :] * forward[j] + 0.5),
                    -level[j],
                    level[j],
                ).astype(BF)
                for j in range(KV)
            ],
            axis=0,
        )
        o_d[...] = o_d[...] * fade + dot(coded, w.astype(BF))
        return carry

    lax.fori_loop(0, 2 * NTILE, step, 0)

    turned = jnp.where(first_head, o_d[0:128, :], o_d[128:256, :])
    high = turned.astype(BF)
    low = (turned - high.astype(F32)).astype(BF)
    sign = h2[0:128, 0:128]
    plain = (dot(sign, high) + dot(sign, low)) * jnp.where(first_head, backward[0], backward[1])
    plain = plain + o_0[...] * jnp.exp2((m_0[...] - m_d[...]) * SCORE)
    dattn[...] = (plain / l_d[...]).T
    total = jnp.zeros((8, 128), F32)
    for h in range(KV * GROUP):
        a = dattn[h * 8 : (h + 1) * 8, :]
        total = total + a * a
    sq_mine[TOK : TOK + 8, :] = jnp.broadcast_to(jnp.sum(total, axis=1, keepdims=True), (8, 128))

    total = jnp.zeros((TOK, 128), F32)
    for kh in range(KV):
        done = (o_p[kh] / l_p[kh]).T
        attn[kh] = done
        for g in range(GROUP):
            a = done[g * TOK : (g + 1) * TOK, :]
            total = total + a * a
    sq_mine[0:TOK, :] = jnp.broadcast_to(jnp.sum(total, axis=1, keepdims=True), (TOK, 128))
    swap = pltpu.make_async_remote_copy(
        src_ref=sq_mine,
        dst_ref=sq_theirs,
        send_sem=g_send,
        recv_sem=g_recv,
        device_id=(s, 1 - grp),
        device_id_type=MESH,
    )
    swap.start()

    for c in ycopies:
        c.wait_send()
    for d in range(7):
        if d > 0:
            wave_copy(d).wait_send()
        to_sibling(d).wait_send()
    swap.wait()
    norm = lax.rsqrt((sq_mine[...] + sq_theirs[...]) / WIDE + EPS)
    for kh in range(KV):
        for g in range(GROUP):
            h = kh * GROUP + g
            out_ref[:, h * HEAD : (h + 1) * HEAD] = (
                attn[kh, g * TOK : (g + 1) * TOK, :] * norm[0:TOK]
            ).astype(BF)
            a = (dattn[h * 8 : (h + 1) * 8, :] * norm[TOK : TOK + 8]).astype(BF)
            for t in range(STEPS):
                dout_ref[t, :, h * HEAD : (h + 1) * HEAD] = a[t * ROWS : (t + 1) * ROWS, :]


def local(q, k, v, mask, widths, exps, dq, nk, nv, ctx):
    vmem = pl.BlockSpec(memory_space=pltpu.VMEM)
    smem = pl.BlockSpec(memory_space=pltpu.SMEM)
    anyw = pl.BlockSpec(memory_space=pl.ANY)
    dma = pltpu.SemaphoreType.DMA
    return pl.pallas_call(
        kernel,
        out_shape=(
            jax.ShapeDtypeStruct(q.shape, BF),
            jax.ShapeDtypeStruct(dq.shape, BF),
        ),
        in_specs=[smem] * 4 + [vmem, anyw, anyw] + [vmem] * 6,
        out_specs=(vmem, vmem),
        scratch_shapes=[
            pltpu.VMEM((2 * OWN, 512), BF),
            pltpu.VMEM((KV, 256, 512), BF),
            pltpu.VMEM((256, 256), BF),
            pltpu.VMEM((256, 256), BF),
            pltpu.VMEM((TILE, 128), BF),
            pltpu.VMEM((TILE, 128), jnp.int32),
            pltpu.VMEM((KV, 1, 512), F32),
            pltpu.VMEM((KV, 1, 512), F32),
            pltpu.VMEM((KV, 128, 512), F32),
            pltpu.VMEM((1, 128), F32),
            pltpu.VMEM((1, 128), F32),
            pltpu.VMEM((256, 128), F32),
            pltpu.VMEM((1, 128), F32),
            pltpu.VMEM((128, 128), F32),
            pltpu.VMEM((128, 128), F32),
            pltpu.VMEM((128, 256), F32),
            pltpu.VMEM((128, 256), F32),
            pltpu.VMEM((KV, 512, 128), F32),
            pltpu.VMEM((128, 128), F32),
            pltpu.VMEM((TOK + 8, 128), F32),
            pltpu.VMEM((TOK + 8, 128), F32),
            dma((4,)),
            dma((2,)),
            dma((2,)),
            dma((7,)),
            dma((7,)),
            dma((7,)),
            dma((7,)),
            dma,
            dma,
        ],
        compiler_params=pltpu.CompilerParams(
            collective_id=0, has_side_effects=True, vmem_limit_bytes=48 * 1024 * 1024
        ),
    )(jnp.asarray(TABLE), widths, exps, ctx, q, k, v, k, v, mask, dq, nk, nv)


def solution(mesh):
    placed = (
        P("seq", "grp"),
        P("seq", "grp"),
        P("seq", "grp"),
        P(),
        P("grp"),
        P("grp"),
        P(None, "seq", "grp"),
        P(None, "seq", "grp"),
        P(None, "seq", "grp"),
        P("seq"),
    )
    return jax.shard_map(
        local,
        mesh=mesh,
        in_specs=placed,
        out_specs=(P("seq", "grp"), P(None, "seq", "grp")),
        check_vma=False,
    )
```

```python
import math

import jax
import jax.numpy as jnp
from jax import lax
from jax.experimental import pallas as pl
from jax.experimental.pallas import tpu as pltpu
from jax.sharding import PartitionSpec as P

HEADS = 32
KV = 2
GROUP = 8
HEAD = 128
STEPS = 4
TOK = 64
ROWS = 2
XS, ZS = 4, 8
HALF = TOK // 2
TILE = 256
VERY_LOW = -1e30
EPS = 1e-6
WIDE = HEADS * HEAD
SCORE = math.log2(math.e) / math.sqrt(HEAD)

BF = jnp.bfloat16
F32 = jnp.float32
MESH = pl.DeviceIdType.MESH

OFFSETS = [(dx, dz) for dx in (0, -1, 1, 2) for dz in (0, -1, 1, -2, 2, -3, 3, 4)]
ORDER = [(0, 0), (1, 0), (0, 1), (2, 0), (1, 1), (3, 0), (2, 1), (4, 0), (3, 1), (5, 0), (4, 1), (6, 0), (5, 1), (6, 1)]
NW = len(ORDER)


def sort_key(path, side):
    far = -9 if side == 0 else 9

    def key(off):
        dx, dz = off
        kx = far if dx == 2 else dx
        kz = far if dz == 4 else dz
        return (kz, kx) if path == 0 else (kx, kz)

    return key


UNITS = {}
SLOT = {}
START = []
for index, (d, side) in enumerate(ORDER):
    START.append(len(SLOT) * HALF)
    for path in (0, 1):
        units = sorted(
            (o for o in OFFSETS if abs(o[0]) + abs(o[1]) == d), key=sort_key(path, side)
        )
        UNITS[(index, path)] = units
        for off in units:
            SLOT[(side, path, *off)] = len(SLOT)
START.append(len(SLOT) * HALF)
OWN = START[-1]
NTILE = OWN // TILE
NEED = [max(k for k in range(NW) if START[k] < (t + 1) * TILE) for t in range(NTILE)]
AFTER = {k: ORDER.index((d + 1, side)) for k, (d, side) in enumerate(ORDER) if d < 6}
TABLE = [
    side * 128 + path * 64 + (dx % XS) * 8 + dz % ZS for (side, path, dx, dz) in SLOT
]


def hops(n, far, side):
    if n == 0:
        return [(1, -1), (-1, 1)]
    if n == far:
        return []
    way = 1 if n < 0 else -1
    if abs(n) == far - 1:
        return [(way, far)] if (way == 1) == (side == 0) else []
    return [(way, n - way)]


def messages(k):
    side = ORDER[k][1]
    out = []
    for path in (0, 1):
        for dx, dz in UNITS[(k, path)]:
            here = SLOT[(side, path, dx, dz)] * HALF
            if path == 0 or dx == 0:
                for way, n in hops(dz, 4, side):
                    out.append((path, "z", way, here, SLOT[(side, path, dx, n)] * HALF))
            if path == 1 or dz == 0:
                for way, n in hops(dx, 2, side):
                    out.append((path, "x", way, here, SLOT[(side, path, n, dz)] * HALF))
    out.sort(key=lambda m: (m[0], m[1], m[2], m[3]))
    merged = []
    for path, axis, way, here, there in out:
        if merged:
            p, a, w, h, t, n = merged[-1]
            if (p, a, w) == (path, axis, way) and h + n == here and t + n == there:
                merged[-1] = (p, a, w, h, t, n + HALF)
                continue
        merged.append((path, axis, way, here, there, HALF))
    merged.sort(key=lambda m: m[0] if m[1] == "z" else 1 - m[0])
    return [m[1:] for m in merged]


def dot(a, b):
    return jnp.dot(a, b, preferred_element_type=F32)


def choose(n, first, values):
    out = jnp.float32(values[0])
    for i, v in enumerate(values[1:]):
        out = jnp.where(n == first + 1 + i, jnp.float32(v), out)
    return out


def kernel(
    q_hbm,
    k_hbm,
    v_hbm,
    mask_hbm,
    widths_hbm,
    exps_hbm,
    dq_hbm,
    nk_hbm,
    nv_hbm,
    ctx_hbm,
    out_ref,
    dout_ref,
    table,
    widths,
    exps,
    ctx,
    q_ref,
    mask_ref,
    dq_ref,
    nk_ref,
    nv_ref,
    kv,
    qx,
    qd,
    h2,
    oh,
    pos,
    m_p,
    l_p,
    o_p,
    m_d,
    l_d,
    o_d,
    m_0,
    o_0,
    dq_s,
    nk_s,
    nv_s,
    attn,
    dattn,
    sq_mine,
    sq_theirs,
    load_sem,
    y_send,
    send_sem,
    recv_sem,
    sib_send,
    sib_recv,
    g_send,
    g_recv,
):
    s = lax.axis_index("seq")
    grp = lax.axis_index("grp")
    core = s % 2
    z = (s // 2) % ZS
    x = (s // (2 * ZS)) % XS
    yh = s // (2 * ZS * XS)

    def at(yh_, x_, z_, core_):
        return ((yh_ * XS + x_) * ZS + z_) * 2 + core_

    peers = {
        ("x", 1): at(yh, (x + 1) % XS, z, core),
        ("x", -1): at(yh, (x + XS - 1) % XS, z, core),
        ("z", 1): at(yh, x, (z + 1) % ZS, core),
        ("z", -1): at(yh, x, (z + ZS - 1) % ZS, core),
    }
    across = at(1 - yh, x, z, core)
    sibling = at(yh, x, z, 1 - core)

    barrier = pltpu.get_barrier_semaphore()
    for dev in (*peers.values(), across, sibling):
        pl.semaphore_signal(barrier, inc=1, device_id=(dev, grp), device_id_type=MESH)
    pl.semaphore_signal(barrier, inc=1, device_id=(s, 1 - grp), device_id_type=MESH)

    loads = [
        pltpu.make_async_copy(src, dst, load_sem.at[i])
        for i, (src, dst) in enumerate(
            (
                (k_hbm, kv.at[pl.ds(0, TOK), pl.ds(0, 256)]),
                (v_hbm, kv.at[pl.ds(0, TOK), pl.ds(256, 256)]),
                (q_hbm, q_ref),
                (mask_hbm, mask_ref),
                (widths_hbm, widths),
                (exps_hbm, exps),
                (ctx_hbm, ctx),
                (dq_hbm, dq_ref),
                (nk_hbm, nk_ref),
                (nv_hbm, nv_ref),
            )
        )
    ]
    for c in loads:
        c.start()

    def remote(src_row, dst_row, count, ssem, rsem, dev):
        return pltpu.make_async_remote_copy(
            src_ref=kv.at[pl.ds(src_row, count), :],
            dst_ref=kv.at[pl.ds(dst_row, count), :],
            send_sem=ssem,
            recv_sem=rsem,
            device_id=(dev, grp),
            device_id_type=MESH,
        )

    def forwards(k):
        if k in AFTER:
            n = AFTER[k]
            for axis, way, here, there, count in messages(k):
                remote(
                    here, there, count, send_sem.at[n], recv_sem.at[n], peers[(axis, way)]
                ).start()

    def wave_copy(k):
        return remote(
            START[k], START[k], START[k + 1] - START[k], send_sem.at[k], recv_sem.at[k], sibling
        )

    def to_sibling(k):
        return remote(
            START[k],
            OWN + START[k],
            START[k + 1] - START[k],
            sib_send.at[k],
            sib_recv.at[k],
            sibling,
        )

    other = ORDER.index((0, 1))
    ycopy = remote(0, START[other], TOK, y_send, recv_sem.at[other], across)
    loads[0].wait()
    loads[1].wait()
    pl.semaphore_wait(barrier, 7)
    ycopy.start()
    forwards(0)
    to_sibling(0).start()
    for i, code in enumerate(TABLE):
        table[i] = code
    for c in loads[2:]:
        c.wait()

    i0 = lax.broadcasted_iota(jnp.int32, (256, 256), 0)
    i1 = lax.broadcasted_iota(jnp.int32, (256, 256), 1)
    both = (i0 & i1) & 127
    parity = jnp.zeros((256, 256), jnp.int32)
    for b in range(7):
        parity = parity + ((both >> b) & 1)
    sign = (1 - 2 * (parity % 2)).astype(F32)
    h2[...] = jnp.where((i0 // 128) == (i1 // 128), sign, 0.0).astype(BF)

    lane = lax.broadcasted_iota(jnp.int32, (1, 128), 1)
    first_head = lane < 64
    level = [choose(widths[i], 3, [3.0, 7.0, 15.0, 31.0, 63.0, 127.0]) for i in range(KV)]
    power = [choose(exps[i], 1, [2.0, 4.0, 8.0, 16.0]) for i in range(KV)]
    inverse = [choose(exps[i], 1, [0.5, 0.25, 0.125, 0.0625]) for i in range(KV)]
    forward = [p / math.sqrt(HEAD) for p in power]
    backward = [p / math.sqrt(HEAD) for p in inverse]
    limits = jnp.where(lane % 2 == 0, ctx[0], ctx[1])

    row = mask_ref[pl.ds(s, 1), :]
    closed = jnp.where((row == 1) & (lane < s), 0.0, VERY_LOW).astype(F32)
    tri = lax.broadcasted_iota(jnp.int32, (TOK, 512), 0) <= (
        lax.broadcasted_iota(jnp.int32, (TOK, 512), 1) % TOK
    )
    for kh in range(KV):
        for g in range(GROUP):
            h = kh * GROUP + g
            piece = q_ref[:, h * HEAD : (h + 1) * HEAD].astype(F32)
            cols = slice(g * TOK, (g + 1) * TOK)
            whole = jnp.concatenate([piece, jnp.broadcast_to(closed, (TOK, 128))], axis=1)
            if g % 2 == 0:
                held = whole
            else:
                two = jnp.concatenate([held, whole], axis=0)
                qx[kh, :, (g - 1) * TOK : (g + 1) * TOK] = two.T.astype(BF)
        sc = dot(kv[0:TOK, kh * HEAD : (kh + 1) * HEAD], qx[kh, 0:128, :])
        sc = jnp.where(tri, sc, VERY_LOW)
        top = jnp.max(sc, axis=0, keepdims=True)
        w = jnp.exp2((sc - top) * SCORE)
        m_p[kh] = top
        l_p[kh] = jnp.sum(w, axis=0, keepdims=True)
        vt = kv[0:TOK, 256 + kh * HEAD : 256 + (kh + 1) * HEAD].astype(F32).T.astype(BF)
        o_p[kh] = dot(vt, w.astype(BF))

    for h in range(KV * GROUP):
        for t in range(STEPS):
            dq_s[h * 8 + t * ROWS : h * 8 + (t + 1) * ROWS, :] = dq_ref[
                t, :, h * HEAD : (h + 1) * HEAD
            ].astype(F32)
    nk_s[...] = jnp.zeros_like(nk_s)
    nv_s[...] = jnp.zeros_like(nv_s)
    for t in range(STEPS):
        nk_s[t * ROWS : (t + 1) * ROWS, :] = nk_ref[t].astype(F32)
        nv_s[t * ROWS : (t + 1) * ROWS, :] = nv_ref[t].astype(F32)
    dq = dq_s[...]
    turned = dot(dq.astype(BF), h2[0:128, 0:128])
    which = lax.broadcasted_iota(jnp.int32, (128, 1), 0) < 64
    turned = (turned * jnp.where(which, backward[0], backward[1])).T
    high = turned.astype(BF).astype(F32)
    low = turned - high
    zero = jnp.zeros((128, 128), F32)
    for part, a in enumerate((high, low)):
        cols = slice(part * 128, (part + 1) * 128)
        qd[0:128, cols] = jnp.where(first_head, a, zero).astype(BF)
        qd[128:256, cols] = jnp.where(first_head, zero, a).astype(BF)
    dqt = dq.T
    upper = jnp.where(first_head, dqt, zero).astype(BF)
    lower = jnp.where(first_head, zero, dqt).astype(BF)
    nk = nk_s[...].astype(BF)
    sc = dot(nk[:, 0:128], upper) + dot(nk[:, 128:256], lower)
    key_i = lax.broadcasted_iota(jnp.int32, (128, 128), 0)
    qry_i = lax.broadcasted_iota(jnp.int32, (128, 128), 1) % (STEPS * ROWS)
    seen = (
        (key_i < STEPS * ROWS)
        & (key_i % ROWS == qry_i % ROWS)
        & (key_i // ROWS <= qry_i // ROWS)
    )
    sc = jnp.where(seen, sc, VERY_LOW)
    top = jnp.max(sc, axis=0, keepdims=True)
    w = jnp.where(seen, jnp.exp2((sc - top) * SCORE), 0.0)
    m_d[...] = top
    m_0[...] = top
    l_d[...] = jnp.sum(w, axis=0, keepdims=True)
    nvt = nv_s[...].T.astype(BF)
    wide = dot(nvt, w.astype(BF))
    o_0[...] = jnp.where(first_head, wide[0:128], wide[128:256])
    o_d[...] = jnp.zeros_like(o_d)

    def step(i, carry):
        done = 0
        for t in range(NTILE):
            waves = range(done + 1, NEED[t] + 1)
            sent = range(done + 1 if t else 0, NEED[t] + 1)
            done = NEED[t]
            if not sent:
                continue

            @pl.when(i == 2 * t)
            def _():
                for k in waves:
                    wave_copy(k).wait_recv()
                    forwards(k)
                    to_sibling(k).start()

            @pl.when(i == 2 * t + 1)
            def _():
                for k in sent:
                    to_sibling(k).wait_recv()

        e = i % 2
        tile = i // 2
        first = pl.multiple_of(e * OWN + tile * TILE, TILE)
        rows_in = lax.broadcasted_iota(jnp.int32, (HALF, 128), 0)
        lanes_in = lax.broadcasted_iota(jnp.int32, (HALF, 128), 1)
        for u in range(TILE // HALF):
            code = table[tile * (TILE // HALF) + u]
            sx = (x + (code % 64) // 8) % XS
            sz = (z + code % 8) % ZS
            block = at((yh + code // 128) % 2, sx, sz, (core + e) % 2)
            here = slice(u * HALF, (u + 1) * HALF)
            oh[here, :] = jnp.where(lanes_in == block, 1.0, 0.0).astype(BF)
            pos[here, :] = rows_in + (block * TOK + (code // 64) % 2 * HALF)

        keys = kv[pl.ds(first, TILE), 0:256]
        vals_t = kv[pl.ds(first, TILE), 256:512].T
        blocks = oh[...]
        for kh in range(KV):
            ext = jnp.concatenate([keys[:, kh * HEAD : (kh + 1) * HEAD], blocks], axis=1)
            sc = dot(ext, qx[kh])
            old = m_p[kh]
            top = jnp.maximum(old, jnp.max(sc, axis=0, keepdims=True))
            w = jnp.exp2(sc * SCORE - top * SCORE)
            fade = jnp.exp2((old - top) * SCORE)
            m_p[kh] = top
            l_p[kh] = l_p[kh] * fade + jnp.sum(w, axis=0, keepdims=True)
            o_p[kh] = o_p[kh] * fade + dot(vals_t[kh * HEAD : (kh + 1) * HEAD, :], w.astype(BF))

        rot = dot(keys, h2[...])
        coded = jnp.concatenate(
            [
                jnp.clip(
                    jnp.floor(rot[:, j * HEAD : (j + 1) * HEAD] * forward[j] + 0.5),
                    -level[j],
                    level[j],
                ).astype(BF)
                for j in range(KV)
            ],
            axis=1,
        )
        two = dot(coded, qd[...])
        sc = jnp.where(pos[...] < limits, two[:, 0:128] + two[:, 128:256], VERY_LOW)
        old = m_d[...]
        top = jnp.maximum(old, jnp.max(sc, axis=0, keepdims=True))
        w = jnp.exp2(sc * SCORE - top * SCORE)
        fade = jnp.exp2((old - top) * SCORE)
        m_d[...] = top
        l_d[...] = l_d[...] * fade + jnp.sum(w, axis=0, keepdims=True)
        rot = dot(h2[...], vals_t)
        coded = jnp.concatenate(
            [
                jnp.clip(
                    jnp.floor(rot[j * HEAD : (j + 1) * HEAD, :] * forward[j] + 0.5),
                    -level[j],
                    level[j],
                ).astype(BF)
                for j in range(KV)
            ],
            axis=0,
        )
        o_d[...] = o_d[...] * fade + dot(coded, w.astype(BF))
        return carry

    lax.fori_loop(0, 2 * NTILE, step, 0)

    turned = jnp.where(first_head, o_d[0:128, :], o_d[128:256, :])
    high = turned.astype(BF)
    low = (turned - high.astype(F32)).astype(BF)
    sign = h2[0:128, 0:128]
    plain = (dot(sign, high) + dot(sign, low)) * jnp.where(first_head, backward[0], backward[1])
    plain = plain + o_0[...] * jnp.exp2((m_0[...] - m_d[...]) * SCORE)
    dattn[...] = (plain / l_d[...]).T
    total = jnp.zeros((8, 128), F32)
    for h in range(KV * GROUP):
        a = dattn[h * 8 : (h + 1) * 8, :]
        total = total + a * a
    sq_mine[TOK : TOK + 8, :] = jnp.broadcast_to(jnp.sum(total, axis=1, keepdims=True), (8, 128))

    total = jnp.zeros((TOK, 128), F32)
    for kh in range(KV):
        done = (o_p[kh] / l_p[kh]).T
        attn[kh] = done
        for g in range(GROUP):
            a = done[g * TOK : (g + 1) * TOK, :]
            total = total + a * a
    sq_mine[0:TOK, :] = jnp.broadcast_to(jnp.sum(total, axis=1, keepdims=True), (TOK, 128))
    swap = pltpu.make_async_remote_copy(
        src_ref=sq_mine,
        dst_ref=sq_theirs,
        send_sem=g_send,
        recv_sem=g_recv,
        device_id=(s, 1 - grp),
        device_id_type=MESH,
    )
    swap.start()

    ycopy.wait_send()
    for k in range(NW):
        if ORDER[k][0] > 0:
            wave_copy(k).wait_send()
        to_sibling(k).wait_send()
    swap.wait()
    norm = lax.rsqrt((sq_mine[...] + sq_theirs[...]) / WIDE + EPS)
    for kh in range(KV):
        for g in range(GROUP):
            h = kh * GROUP + g
            out_ref[:, h * HEAD : (h + 1) * HEAD] = (
                attn[kh, g * TOK : (g + 1) * TOK, :] * norm[0:TOK]
            ).astype(BF)
            a = (dattn[h * 8 : (h + 1) * 8, :] * norm[TOK : TOK + 8]).astype(BF)
            for t in range(STEPS):
                dout_ref[t, :, h * HEAD : (h + 1) * HEAD] = a[t * ROWS : (t + 1) * ROWS, :]


def local(q, k, v, mask, widths, exps, dq, nk, nv, ctx):
    vmem = pl.BlockSpec(memory_space=pltpu.VMEM)
    hbm = pl.BlockSpec(memory_space=pltpu.HBM)
    dma = pltpu.SemaphoreType.DMA
    return pl.pallas_call(
        kernel,
        out_shape=(
            jax.ShapeDtypeStruct(q.shape, BF),
            jax.ShapeDtypeStruct(dq.shape, BF),
        ),
        in_specs=[hbm] * 10,
        out_specs=(vmem, vmem),
        scratch_shapes=[
            pltpu.SMEM((len(TABLE),), jnp.int32),
            pltpu.SMEM((KV,), jnp.int32),
            pltpu.SMEM((KV,), jnp.int32),
            pltpu.SMEM((ROWS,), jnp.int32),
            pltpu.VMEM(q.shape, BF),
            pltpu.VMEM(mask.shape, jnp.int32),
            pltpu.VMEM(dq.shape, BF),
            pltpu.VMEM(nk.shape, BF),
            pltpu.VMEM(nv.shape, BF),
            pltpu.VMEM((2 * OWN, 512), BF),
            pltpu.VMEM((KV, 256, 512), BF),
            pltpu.VMEM((256, 256), BF),
            pltpu.VMEM((256, 256), BF),
            pltpu.VMEM((TILE, 128), BF),
            pltpu.VMEM((TILE, 128), jnp.int32),
            pltpu.VMEM((KV, 1, 512), F32),
            pltpu.VMEM((KV, 1, 512), F32),
            pltpu.VMEM((KV, 128, 512), F32),
            pltpu.VMEM((1, 128), F32),
            pltpu.VMEM((1, 128), F32),
            pltpu.VMEM((256, 128), F32),
            pltpu.VMEM((1, 128), F32),
            pltpu.VMEM((128, 128), F32),
            pltpu.VMEM((128, 128), F32),
            pltpu.VMEM((128, 256), F32),
            pltpu.VMEM((128, 256), F32),
            pltpu.VMEM((KV, 512, 128), F32),
            pltpu.VMEM((128, 128), F32),
            pltpu.VMEM((TOK + 8, 128), F32),
            pltpu.VMEM((TOK + 8, 128), F32),
            dma((10,)),
            dma,
            dma((NW,)),
            dma((NW,)),
            dma((NW,)),
            dma((NW,)),
            dma,
            dma,
        ],
        compiler_params=pltpu.CompilerParams(
            collective_id=0, has_side_effects=True, vmem_limit_bytes=48 * 1024 * 1024
        ),
    )(q, k, v, mask, widths, exps, dq, nk, nv, ctx)


def solution(mesh):
    placed = (
        P("seq", "grp"),
        P("seq", "grp"),
        P("seq", "grp"),
        P(),
        P("grp"),
        P("grp"),
        P(None, "seq", "grp"),
        P(None, "seq", "grp"),
        P(None, "seq", "grp"),
        P("seq"),
    )
    return jax.shard_map(
        local,
        mesh=mesh,
        in_specs=placed,
        out_specs=(P("seq", "grp"), P(None, "seq", "grp")),
        check_vma=False,
    )
```

```python
import math

import jax
import jax.numpy as jnp
from jax import lax
from jax.experimental import pallas as pl
from jax.experimental.pallas import tpu as pltpu
from jax.sharding import PartitionSpec as P

HEADS = 32
KV = 2
GROUP = 8
HEAD = 128
STEPS = 4
TOK = 64
ROWS = 2
XS, ZS = 4, 8
HALF = TOK // 2
TILE = 512
VERY_LOW = -1e30
EPS = 1e-6
WIDE = HEADS * HEAD
SCORE = math.log2(math.e) / math.sqrt(HEAD)

BF = jnp.bfloat16
F32 = jnp.float32
MESH = pl.DeviceIdType.MESH

OFFSETS = [(dx, dz) for dx in (0, -1, 1, 2) for dz in (0, -1, 1, -2, 2, -3, 3, 4)]
ORDER = [(0, 0), (1, 0), (0, 1), (2, 0), (1, 1), (3, 0), (2, 1), (4, 0), (3, 1), (5, 0), (4, 1), (6, 0), (5, 1), (6, 1)]
NW = len(ORDER)


def sort_key(path, side):
    far = -9 if side == 0 else 9

    def key(off):
        dx, dz = off
        kx = far if dx == 2 else dx
        kz = far if dz == 4 else dz
        return (kz, kx) if path == 0 else (kx, kz)

    return key


UNITS = {}
SLOT = {}
START = []
for index, (d, side) in enumerate(ORDER):
    START.append(len(SLOT) * HALF)
    for path in (0, 1):
        units = sorted(
            (o for o in OFFSETS if abs(o[0]) + abs(o[1]) == d), key=sort_key(path, side)
        )
        UNITS[(index, path)] = units
        for off in units:
            SLOT[(side, path, *off)] = len(SLOT)
START.append(len(SLOT) * HALF)
OWN = START[-1]
NTILE = OWN // TILE
NEED = [max(k for k in range(NW) if START[k] < (t + 1) * TILE) for t in range(NTILE)]
AFTER = {k: ORDER.index((d + 1, side)) for k, (d, side) in enumerate(ORDER) if d < 6}
TABLE = [
    side * 128 + path * 64 + (dx % XS) * 8 + dz % ZS for (side, path, dx, dz) in SLOT
]


def hops(n, far, side):
    if n == 0:
        return [(1, -1), (-1, 1)]
    if n == far:
        return []
    way = 1 if n < 0 else -1
    if abs(n) == far - 1:
        return [(way, far)] if (way == 1) == (side == 0) else []
    return [(way, n - way)]


def messages(k):
    side = ORDER[k][1]
    out = []
    for path in (0, 1):
        for dx, dz in UNITS[(k, path)]:
            here = SLOT[(side, path, dx, dz)] * HALF
            if path == 0 or dx == 0:
                for way, n in hops(dz, 4, side):
                    out.append((path, "z", way, here, SLOT[(side, path, dx, n)] * HALF))
            if path == 1 or dz == 0:
                for way, n in hops(dx, 2, side):
                    out.append((path, "x", way, here, SLOT[(side, path, n, dz)] * HALF))
    out.sort(key=lambda m: (m[0], m[1], m[2], m[3]))
    merged = []
    for path, axis, way, here, there in out:
        if merged:
            p, a, w, h, t, n = merged[-1]
            if (p, a, w) == (path, axis, way) and h + n == here and t + n == there:
                merged[-1] = (p, a, w, h, t, n + HALF)
                continue
        merged.append((path, axis, way, here, there, HALF))
    merged.sort(key=lambda m: m[0] if m[1] == "z" else 1 - m[0])
    return [m[1:] for m in merged]


def dot(a, b):
    return jnp.dot(a, b, preferred_element_type=F32)


def choose(n, first, values):
    out = jnp.float32(values[0])
    for i, v in enumerate(values[1:]):
        out = jnp.where(n == first + 1 + i, jnp.float32(v), out)
    return out


def kernel(
    q_hbm,
    k_hbm,
    v_hbm,
    mask_hbm,
    widths_hbm,
    exps_hbm,
    dq_hbm,
    nk_hbm,
    nv_hbm,
    ctx_hbm,
    out_ref,
    dout_ref,
    table,
    widths,
    exps,
    ctx,
    q_ref,
    mask_ref,
    dq_ref,
    nk_ref,
    nv_ref,
    kv,
    qx,
    qd,
    h2,
    oh,
    pos,
    m_p,
    l_p,
    o_p,
    m_d,
    l_d,
    o_d,
    m_0,
    o_0,
    dq_s,
    nk_s,
    nv_s,
    attn,
    dattn,
    sq_mine,
    sq_theirs,
    load_sem,
    y_send,
    send_sem,
    recv_sem,
    sib_send,
    sib_recv,
    g_send,
    g_recv,
):
    s = lax.axis_index("seq")
    grp = lax.axis_index("grp")
    core = s % 2
    z = (s // 2) % ZS
    x = (s // (2 * ZS)) % XS
    yh = s // (2 * ZS * XS)

    def at(yh_, x_, z_, core_):
        return ((yh_ * XS + x_) * ZS + z_) * 2 + core_

    peers = {
        ("x", 1): at(yh, (x + 1) % XS, z, core),
        ("x", -1): at(yh, (x + XS - 1) % XS, z, core),
        ("z", 1): at(yh, x, (z + 1) % ZS, core),
        ("z", -1): at(yh, x, (z + ZS - 1) % ZS, core),
    }
    across = at(1 - yh, x, z, core)
    sibling = at(yh, x, z, 1 - core)

    barrier = pltpu.get_barrier_semaphore()
    for dev in (*peers.values(), across, sibling):
        pl.semaphore_signal(barrier, inc=1, device_id=(dev, grp), device_id_type=MESH)
    pl.semaphore_signal(barrier, inc=1, device_id=(s, 1 - grp), device_id_type=MESH)

    loads = [
        pltpu.make_async_copy(src, dst, load_sem.at[i])
        for i, (src, dst) in enumerate(
            (
                (k_hbm, kv.at[pl.ds(0, TOK), pl.ds(0, 256)]),
                (v_hbm, kv.at[pl.ds(0, TOK), pl.ds(256, 256)]),
                (q_hbm, q_ref),
                (mask_hbm, mask_ref),
                (widths_hbm, widths),
                (exps_hbm, exps),
                (ctx_hbm, ctx),
                (dq_hbm, dq_ref),
                (nk_hbm, nk_ref),
                (nv_hbm, nv_ref),
            )
        )
    ]
    for c in loads:
        c.start()

    def remote(src_row, dst_row, count, ssem, rsem, dev):
        return pltpu.make_async_remote_copy(
            src_ref=kv.at[pl.ds(src_row, count), :],
            dst_ref=kv.at[pl.ds(dst_row, count), :],
            send_sem=ssem,
            recv_sem=rsem,
            device_id=(dev, grp),
            device_id_type=MESH,
        )

    def forwards(k):
        if k in AFTER:
            n = AFTER[k]
            for axis, way, here, there, count in messages(k):
                remote(
                    here, there, count, send_sem.at[n], recv_sem.at[n], peers[(axis, way)]
                ).start()

    def wave_copy(k):
        return remote(
            START[k], START[k], START[k + 1] - START[k], send_sem.at[k], recv_sem.at[k], sibling
        )

    def to_sibling(k):
        return remote(
            START[k],
            OWN + START[k],
            START[k + 1] - START[k],
            sib_send.at[k],
            sib_recv.at[k],
            sibling,
        )

    other = ORDER.index((0, 1))
    ycopy = remote(0, START[other], TOK, y_send, recv_sem.at[other], across)
    loads[0].wait()
    loads[1].wait()
    pl.semaphore_wait(barrier, 7)
    ycopy.start()
    forwards(0)
    to_sibling(0).start()
    for i, code in enumerate(TABLE):
        table[i] = code
    for c in loads[2:]:
        c.wait()

    i0 = lax.broadcasted_iota(jnp.int32, (256, 256), 0)
    i1 = lax.broadcasted_iota(jnp.int32, (256, 256), 1)
    both = (i0 & i1) & 127
    parity = jnp.zeros((256, 256), jnp.int32)
    for b in range(7):
        parity = parity + ((both >> b) & 1)
    sign = (1 - 2 * (parity % 2)).astype(F32)
    h2[...] = jnp.where((i0 // 128) == (i1 // 128), sign, 0.0).astype(BF)

    lane = lax.broadcasted_iota(jnp.int32, (1, 128), 1)
    first_head = lane < 64
    level = [choose(widths[i], 3, [3.0, 7.0, 15.0, 31.0, 63.0, 127.0]) for i in range(KV)]
    power = [choose(exps[i], 1, [2.0, 4.0, 8.0, 16.0]) for i in range(KV)]
    inverse = [choose(exps[i], 1, [0.5, 0.25, 0.125, 0.0625]) for i in range(KV)]
    forward = [p / math.sqrt(HEAD) for p in power]
    backward = [p / math.sqrt(HEAD) for p in inverse]
    limits = jnp.where(lane % 2 == 0, ctx[0], ctx[1])

    row = mask_ref[pl.ds(s, 1), :]
    closed = jnp.where((row == 1) & (lane < s), 0.0, VERY_LOW).astype(F32)
    tri = lax.broadcasted_iota(jnp.int32, (TOK, 512), 0) <= (
        lax.broadcasted_iota(jnp.int32, (TOK, 512), 1) % TOK
    )
    for kh in range(KV):
        for g in range(GROUP):
            h = kh * GROUP + g
            piece = q_ref[:, h * HEAD : (h + 1) * HEAD].astype(F32)
            cols = slice(g * TOK, (g + 1) * TOK)
            whole = jnp.concatenate([piece, jnp.broadcast_to(closed, (TOK, 128))], axis=1)
            if g % 2 == 0:
                held = whole
            else:
                two = jnp.concatenate([held, whole], axis=0)
                qx[kh, :, (g - 1) * TOK : (g + 1) * TOK] = two.T.astype(BF)
        sc = dot(kv[0:TOK, kh * HEAD : (kh + 1) * HEAD], qx[kh, 0:128, :])
        sc = jnp.where(tri, sc, VERY_LOW)
        top = jnp.max(sc, axis=0, keepdims=True)
        w = jnp.exp2((sc - top) * SCORE)
        m_p[kh] = top
        l_p[kh] = jnp.sum(w, axis=0, keepdims=True)
        vt = kv[0:TOK, 256 + kh * HEAD : 256 + (kh + 1) * HEAD].astype(F32).T.astype(BF)
        o_p[kh] = dot(vt, w.astype(BF))

    for h in range(KV * GROUP):
        for t in range(STEPS):
            dq_s[h * 8 + t * ROWS : h * 8 + (t + 1) * ROWS, :] = dq_ref[
                t, :, h * HEAD : (h + 1) * HEAD
            ].astype(F32)
    nk_s[...] = jnp.zeros_like(nk_s)
    nv_s[...] = jnp.zeros_like(nv_s)
    for t in range(STEPS):
        nk_s[t * ROWS : (t + 1) * ROWS, :] = nk_ref[t].astype(F32)
        nv_s[t * ROWS : (t + 1) * ROWS, :] = nv_ref[t].astype(F32)
    dq = dq_s[...]
    turned = dot(dq.astype(BF), h2[0:128, 0:128])
    which = lax.broadcasted_iota(jnp.int32, (128, 1), 0) < 64
    turned = (turned * jnp.where(which, backward[0], backward[1])).T
    high = turned.astype(BF).astype(F32)
    low = turned - high
    zero = jnp.zeros((128, 128), F32)
    for part, a in enumerate((high, low)):
        cols = slice(part * 128, (part + 1) * 128)
        qd[0:128, cols] = jnp.where(first_head, a, zero).astype(BF)
        qd[128:256, cols] = jnp.where(first_head, zero, a).astype(BF)
    dqt = dq.T
    upper = jnp.where(first_head, dqt, zero).astype(BF)
    lower = jnp.where(first_head, zero, dqt).astype(BF)
    nk = nk_s[...].astype(BF)
    sc = dot(nk[:, 0:128], upper) + dot(nk[:, 128:256], lower)
    key_i = lax.broadcasted_iota(jnp.int32, (128, 128), 0)
    qry_i = lax.broadcasted_iota(jnp.int32, (128, 128), 1) % (STEPS * ROWS)
    seen = (
        (key_i < STEPS * ROWS)
        & (key_i % ROWS == qry_i % ROWS)
        & (key_i // ROWS <= qry_i // ROWS)
    )
    sc = jnp.where(seen, sc, VERY_LOW)
    top = jnp.max(sc, axis=0, keepdims=True)
    w = jnp.where(seen, jnp.exp2((sc - top) * SCORE), 0.0)
    m_d[...] = top
    m_0[...] = top
    l_d[...] = jnp.sum(w, axis=0, keepdims=True)
    nvt = nv_s[...].T.astype(BF)
    wide = dot(nvt, w.astype(BF))
    o_0[...] = jnp.where(first_head, wide[0:128], wide[128:256])
    o_d[...] = jnp.zeros_like(o_d)

    def compute(e, tile):
        first = pl.multiple_of(e * OWN + tile * TILE, TILE)
        rows_in = lax.broadcasted_iota(jnp.int32, (HALF, 128), 0)
        lanes_in = lax.broadcasted_iota(jnp.int32, (HALF, 128), 1)
        for u in range(TILE // HALF):
            code = table[tile * (TILE // HALF) + u]
            sx = (x + (code % 64) // 8) % XS
            sz = (z + code % 8) % ZS
            block = at((yh + code // 128) % 2, sx, sz, (core + e) % 2)
            here = slice(u * HALF, (u + 1) * HALF)
            oh[here, :] = jnp.where(lanes_in == block, 1.0, 0.0).astype(BF)
            pos[here, :] = rows_in + (block * TOK + (code // 64) % 2 * HALF)

        keys = kv[pl.ds(first, TILE), 0:256]
        vals_t = kv[pl.ds(first, TILE), 256:512].T
        blocks = oh[...]
        for kh in range(KV):
            ext = jnp.concatenate([keys[:, kh * HEAD : (kh + 1) * HEAD], blocks], axis=1)
            sc = dot(ext, qx[kh])
            old = m_p[kh]
            top = jnp.maximum(old, jnp.max(sc, axis=0, keepdims=True))
            w = jnp.exp2(sc * SCORE - top * SCORE)
            fade = jnp.exp2((old - top) * SCORE)
            m_p[kh] = top
            l_p[kh] = l_p[kh] * fade + jnp.sum(w, axis=0, keepdims=True)
            o_p[kh] = o_p[kh] * fade + dot(vals_t[kh * HEAD : (kh + 1) * HEAD, :], w.astype(BF))

        rot = dot(keys, h2[...])
        coded = jnp.concatenate(
            [
                jnp.clip(
                    jnp.floor(rot[:, j * HEAD : (j + 1) * HEAD] * forward[j] + 0.5),
                    -level[j],
                    level[j],
                ).astype(BF)
                for j in range(KV)
            ],
            axis=1,
        )
        two = dot(coded, qd[...])
        sc = jnp.where(pos[...] < limits, two[:, 0:128] + two[:, 128:256], VERY_LOW)
        old = m_d[...]
        top = jnp.maximum(old, jnp.max(sc, axis=0, keepdims=True))
        w = jnp.exp2(sc * SCORE - top * SCORE)
        fade = jnp.exp2((old - top) * SCORE)
        m_d[...] = top
        l_d[...] = l_d[...] * fade + jnp.sum(w, axis=0, keepdims=True)
        rot = dot(h2[...], vals_t)
        coded = jnp.concatenate(
            [
                jnp.clip(
                    jnp.floor(rot[j * HEAD : (j + 1) * HEAD, :] * forward[j] + 0.5),
                    -level[j],
                    level[j],
                ).astype(BF)
                for j in range(KV)
            ],
            axis=0,
        )
        o_d[...] = o_d[...] * fade + dot(coded, w.astype(BF))

    for k in range(1, NW + 1):
        if k < NW:
            wave_copy(k).wait_recv()
            forwards(k)
            to_sibling(k).start()
        to_sibling(k - 1).wait_recv()
        mine = [t for t in range(NTILE) if NEED[t] == k]
        theirs = [t for t in range(NTILE) if NEED[t] == k - 1]
        n_theirs, n_all = len(theirs), len(theirs) + len(mine)
        if not n_all:
            continue
        t_theirs, t_mine = (theirs or [0])[0], (mine or [0])[0]

        def step(j, carry):
            e = jnp.where(j < n_theirs, 1, 0)
            compute(e, jnp.where(j < n_theirs, t_theirs + j, t_mine + j - n_theirs))
            return carry

        lax.fori_loop(0, n_all, step, 0)

    turned = jnp.where(first_head, o_d[0:128, :], o_d[128:256, :])
    high = turned.astype(BF)
    low = (turned - high.astype(F32)).astype(BF)
    sign = h2[0:128, 0:128]
    plain = (dot(sign, high) + dot(sign, low)) * jnp.where(first_head, backward[0], backward[1])
    plain = plain + o_0[...] * jnp.exp2((m_0[...] - m_d[...]) * SCORE)
    dattn[...] = (plain / l_d[...]).T
    total = jnp.zeros((8, 128), F32)
    for h in range(KV * GROUP):
        a = dattn[h * 8 : (h + 1) * 8, :]
        total = total + a * a
    sq_mine[TOK : TOK + 8, :] = jnp.broadcast_to(jnp.sum(total, axis=1, keepdims=True), (8, 128))

    total = jnp.zeros((TOK, 128), F32)
    for kh in range(KV):
        done = (o_p[kh] / l_p[kh]).T
        attn[kh] = done
        for g in range(GROUP):
            a = done[g * TOK : (g + 1) * TOK, :]
            total = total + a * a
    sq_mine[0:TOK, :] = jnp.broadcast_to(jnp.sum(total, axis=1, keepdims=True), (TOK, 128))
    swap = pltpu.make_async_remote_copy(
        src_ref=sq_mine,
        dst_ref=sq_theirs,
        send_sem=g_send,
        recv_sem=g_recv,
        device_id=(s, 1 - grp),
        device_id_type=MESH,
    )
    swap.start()

    ycopy.wait_send()
    for k in range(NW):
        if ORDER[k][0] > 0:
            wave_copy(k).wait_send()
        to_sibling(k).wait_send()
    swap.wait()
    norm = lax.rsqrt((sq_mine[...] + sq_theirs[...]) / WIDE + EPS)
    for kh in range(KV):
        for g in range(GROUP):
            h = kh * GROUP + g
            out_ref[:, h * HEAD : (h + 1) * HEAD] = (
                attn[kh, g * TOK : (g + 1) * TOK, :] * norm[0:TOK]
            ).astype(BF)
            a = (dattn[h * 8 : (h + 1) * 8, :] * norm[TOK : TOK + 8]).astype(BF)
            for t in range(STEPS):
                dout_ref[t, :, h * HEAD : (h + 1) * HEAD] = a[t * ROWS : (t + 1) * ROWS, :]


def local(q, k, v, mask, widths, exps, dq, nk, nv, ctx):
    vmem = pl.BlockSpec(memory_space=pltpu.VMEM)
    hbm = pl.BlockSpec(memory_space=pltpu.HBM)
    dma = pltpu.SemaphoreType.DMA
    return pl.pallas_call(
        kernel,
        out_shape=(
            jax.ShapeDtypeStruct(q.shape, BF),
            jax.ShapeDtypeStruct(dq.shape, BF),
        ),
        in_specs=[hbm] * 10,
        out_specs=(vmem, vmem),
        scratch_shapes=[
            pltpu.SMEM((len(TABLE),), jnp.int32),
            pltpu.SMEM((KV,), jnp.int32),
            pltpu.SMEM((KV,), jnp.int32),
            pltpu.SMEM((ROWS,), jnp.int32),
            pltpu.VMEM(q.shape, BF),
            pltpu.VMEM(mask.shape, jnp.int32),
            pltpu.VMEM(dq.shape, BF),
            pltpu.VMEM(nk.shape, BF),
            pltpu.VMEM(nv.shape, BF),
            pltpu.VMEM((2 * OWN, 512), BF),
            pltpu.VMEM((KV, 256, 512), BF),
            pltpu.VMEM((256, 256), BF),
            pltpu.VMEM((256, 256), BF),
            pltpu.VMEM((TILE, 128), BF),
            pltpu.VMEM((TILE, 128), jnp.int32),
            pltpu.VMEM((KV, 1, 512), F32),
            pltpu.VMEM((KV, 1, 512), F32),
            pltpu.VMEM((KV, 128, 512), F32),
            pltpu.VMEM((1, 128), F32),
            pltpu.VMEM((1, 128), F32),
            pltpu.VMEM((256, 128), F32),
            pltpu.VMEM((1, 128), F32),
            pltpu.VMEM((128, 128), F32),
            pltpu.VMEM((128, 128), F32),
            pltpu.VMEM((128, 256), F32),
            pltpu.VMEM((128, 256), F32),
            pltpu.VMEM((KV, 512, 128), F32),
            pltpu.VMEM((128, 128), F32),
            pltpu.VMEM((TOK + 8, 128), F32),
            pltpu.VMEM((TOK + 8, 128), F32),
            dma((10,)),
            dma,
            dma((NW,)),
            dma((NW,)),
            dma((NW,)),
            dma((NW,)),
            dma,
            dma,
        ],
        compiler_params=pltpu.CompilerParams(
            collective_id=0, has_side_effects=True, vmem_limit_bytes=67_043_328
        ),
    )(q, k, v, mask, widths, exps, dq, nk, nv, ctx)


def solution(mesh):
    placed = (
        P("seq", "grp"),
        P("seq", "grp"),
        P("seq", "grp"),
        P(),
        P("grp"),
        P("grp"),
        P(None, "seq", "grp"),
        P(None, "seq", "grp"),
        P(None, "seq", "grp"),
        P("seq"),
    )
    return jax.shard_map(
        local,
        mesh=mesh,
        in_specs=placed,
        out_specs=(P("seq", "grp"), P(None, "seq", "grp")),
        check_vma=False,
    )
```

```python
import math

import jax
import jax.numpy as jnp
from jax import lax
from jax.experimental import pallas as pl
from jax.experimental.pallas import tpu as pltpu
from jax.sharding import PartitionSpec as P

HEADS = 32
KV = 2
GROUP = 8
HEAD = 128
STEPS = 4
TOK = 64
ROWS = 2
XS, ZS = 4, 8
HALF = TOK // 2
TILE = 512
VERY_LOW = -1e30
EPS = 1e-6
WIDE = HEADS * HEAD
SCORE = math.log2(math.e) / math.sqrt(HEAD)

BF = jnp.bfloat16
F32 = jnp.float32
MESH = pl.DeviceIdType.MESH

PLAN = [
    ((0, 0, 0), []),
    ((0, 0, 1), []),
    ((1, 0, 0), []),
    ((1, 0, 1), []),
    ((0, 1, 0), []),
    ((0, 1, 1), []),
    ((2, 0, 0), [(0, 0)]),
    ((2, 0, 1), []),
    ((1, 1, 0), [(1, 0)]),
    ((1, 1, 1), [(0, 1), (1, 1)]),
    ((3, 0, 0), []),
    ((3, 0, 1), [(0, 2)]),
    ((2, 1, 0), []),
    ((2, 1, 1), [(1, 2), (0, 3), (1, 3)]),
    ((4, 0, 0), []),
    ((4, 0, 1), []),
    ((3, 1, 0), [(0, 4)]),
    ((3, 1, 1), [(1, 4)]),
    ((5, 0, 1), []),
    ((5, 0, 0), [(0, 5), (1, 5)]),
    ((4, 1, 0), []),
    ((6, 0, 1), []),
    ((4, 1, 1), []),
    ((6, 0, 0), [(0, 6), (1, 6)]),
    ((5, 1, 0), []),
    ((5, 1, 1), []),
    ((6, 1, 0), []),
    ((6, 1, 1), [(0, 7), (1, 7)]),
]
ORDER = [g for g, _ in PLAN]
NW = len(ORDER)
OFFSETS = [(dx, dz) for dx in (0, -1, 1, 2) for dz in (0, -1, 1, -2, 2, -3, 3, 4)]


def sort_key(path, side):
    far = -9 if side == 0 else 9

    def key(off):
        dx, dz = off
        kx = far if dx == 2 else dx
        kz = far if dz == 4 else dz
        return (kz, kx) if path == 0 else (kx, kz)

    return key


UNITS = []
SLOT = {}
START = []
for d, side, path in ORDER:
    START.append(len(SLOT) * HALF)
    UNITS.append(
        sorted((o for o in OFFSETS if abs(o[0]) + abs(o[1]) == d), key=sort_key(path, side))
    )
    for off in UNITS[-1]:
        SLOT[(side, path, *off)] = len(SLOT)
START.append(len(SLOT) * HALF)
SOURCES = list(SLOT)
OWN = START[-1]
NTILE = OWN // TILE
NEED = [max(k for k in range(NW) if START[k] < (t + 1) * TILE) for t in range(NTILE)]
AFTER = {k: ORDER.index((d + 1, side, path)) for k, (d, side, path) in enumerate(ORDER) if d < 6}


def hops(n, far, side):
    if n == 0:
        return [(1, -1), (-1, 1)]
    if n == far:
        return []
    way = 1 if n < 0 else -1
    if abs(n) == far - 1:
        return [(way, far)] if (way == 1) == (side == 0) else []
    return [(way, n - way)]


def messages(k):
    _, side, path = ORDER[k]
    out = []
    for dx, dz in UNITS[k]:
        here = SLOT[(side, path, dx, dz)] * HALF
        if path == 0 or dx == 0:
            for way, n in hops(dz, 4, side):
                out.append((path, "z", way, here, SLOT[(side, path, dx, n)] * HALF))
        if path == 1 or dz == 0:
            for way, n in hops(dx, 2, side):
                out.append((path, "x", way, here, SLOT[(side, path, n, dz)] * HALF))
    out.sort(key=lambda m: (m[0], m[1], m[2], m[3]))
    merged = []
    for path, axis, way, here, there in out:
        if merged:
            p, a, w, h, t, n = merged[-1]
            if (p, a, w) == (path, axis, way) and h + n == here and t + n == there:
                merged[-1] = (p, a, w, h, t, n + HALF)
                continue
        merged.append((path, axis, way, here, there, HALF))
    merged.sort(key=lambda m: m[0] if m[1] == "z" else 1 - m[0])
    return [m[1:] for m in merged]


def dot(a, b):
    return jnp.dot(a, b, preferred_element_type=F32)


def choose(n, first, values):
    out = jnp.float32(values[0])
    for i, v in enumerate(values[1:]):
        out = jnp.where(n == first + 1 + i, jnp.float32(v), out)
    return out


def kernel(
    q_hbm,
    k_hbm,
    v_hbm,
    mask_hbm,
    widths_hbm,
    exps_hbm,
    dq_hbm,
    nk_hbm,
    nv_hbm,
    ctx_hbm,
    out_ref,
    dout_ref,
    widths,
    exps,
    ctx,
    q_ref,
    mask_ref,
    dq_ref,
    nk_ref,
    nv_ref,
    kv,
    qx,
    qd,
    h2,
    oh,
    pos,
    m_p,
    l_p,
    o_p,
    m_d,
    l_d,
    o_d,
    m_0,
    o_0,
    dq_s,
    nk_s,
    nv_s,
    attn,
    dattn,
    sq_mine,
    sq_theirs,
    load_sem,
    y_send,
    send_sem,
    recv_sem,
    sib_send,
    sib_recv,
    g_send,
    g_recv,
):
    s = lax.axis_index("seq")
    grp = lax.axis_index("grp")
    core = s % 2
    z = (s // 2) % ZS
    x = (s // (2 * ZS)) % XS
    yh = s // (2 * ZS * XS)

    def at(yh_, x_, z_, core_):
        return ((yh_ * XS + x_) * ZS + z_) * 2 + core_

    peers = {
        ("x", 1): at(yh, (x + 1) % XS, z, core),
        ("x", -1): at(yh, (x + XS - 1) % XS, z, core),
        ("z", 1): at(yh, x, (z + 1) % ZS, core),
        ("z", -1): at(yh, x, (z + ZS - 1) % ZS, core),
    }
    across = at(1 - yh, x, z, core)
    sibling = at(yh, x, z, 1 - core)

    barrier = pltpu.get_barrier_semaphore()
    for dev in (*peers.values(), across, sibling):
        pl.semaphore_signal(barrier, inc=1, device_id=(dev, grp), device_id_type=MESH)
    pl.semaphore_signal(barrier, inc=1, device_id=(s, 1 - grp), device_id_type=MESH)

    loads = [
        pltpu.make_async_copy(src, dst, load_sem.at[i])
        for i, (src, dst) in enumerate(
            (
                (k_hbm, kv.at[pl.ds(0, TOK), pl.ds(0, 256)]),
                (v_hbm, kv.at[pl.ds(0, TOK), pl.ds(256, 256)]),
                (q_hbm, q_ref),
                (mask_hbm, mask_ref),
                (widths_hbm, widths),
                (exps_hbm, exps),
                (ctx_hbm, ctx),
                (dq_hbm, dq_ref),
                (nk_hbm, nk_ref),
                (nv_hbm, nv_ref),
            )
        )
    ]
    for c in loads:
        c.start()

    def remote(src_row, dst_row, count, ssem, rsem, dev):
        return pltpu.make_async_remote_copy(
            src_ref=kv.at[pl.ds(src_row, count), :],
            dst_ref=kv.at[pl.ds(dst_row, count), :],
            send_sem=ssem,
            recv_sem=rsem,
            device_id=(dev, grp),
            device_id_type=MESH,
        )

    def forwards(k):
        if k in AFTER:
            n = AFTER[k]
            for axis, way, here, there, count in messages(k):
                remote(
                    here, there, count, send_sem.at[n], recv_sem.at[n], peers[(axis, way)]
                ).start()

    def wave_copy(k):
        return remote(
            START[k], START[k], START[k + 1] - START[k], send_sem.at[k], recv_sem.at[k], sibling
        )

    def to_sibling(k):
        return remote(
            START[k],
            OWN + START[k],
            START[k + 1] - START[k],
            sib_send.at[k],
            sib_recv.at[k],
            sibling,
        )

    theirs = [ORDER.index((0, 1, path)) for path in (0, 1)]
    ycopies = [
        remote(path * HALF, START[k], HALF, y_send.at[path], recv_sem.at[k], across)
        for path, k in enumerate(theirs)
    ]
    loads[0].wait()
    loads[1].wait()
    pl.semaphore_wait(barrier, 7)
    for c in ycopies:
        c.start()
    for k in (0, 1):
        forwards(k)
        to_sibling(k).start()
    for c in loads[2:]:
        c.wait()

    i0 = lax.broadcasted_iota(jnp.int32, (256, 256), 0)
    i1 = lax.broadcasted_iota(jnp.int32, (256, 256), 1)
    both = (i0 & i1) & 127
    parity = jnp.zeros((256, 256), jnp.int32)
    for b in range(7):
        parity = parity + ((both >> b) & 1)
    sign = (1 - 2 * (parity % 2)).astype(F32)
    h2[...] = jnp.where((i0 // 128) == (i1 // 128), sign, 0.0).astype(BF)

    lane = lax.broadcasted_iota(jnp.int32, (1, 128), 1)
    first_head = lane < 64
    level = [choose(widths[i], 3, [3.0, 7.0, 15.0, 31.0, 63.0, 127.0]) for i in range(KV)]
    power = [choose(exps[i], 1, [2.0, 4.0, 8.0, 16.0]) for i in range(KV)]
    inverse = [choose(exps[i], 1, [0.5, 0.25, 0.125, 0.0625]) for i in range(KV)]
    forward = [p / math.sqrt(HEAD) for p in power]
    backward = [p / math.sqrt(HEAD) for p in inverse]
    limits = jnp.where(lane % 2 == 0, ctx[0], ctx[1])

    row = mask_ref[pl.ds(s, 1), :]
    closed = jnp.where((row == 1) & (lane < s), 0.0, VERY_LOW).astype(F32)
    tri = lax.broadcasted_iota(jnp.int32, (TOK, 512), 0) <= (
        lax.broadcasted_iota(jnp.int32, (TOK, 512), 1) % TOK
    )
    for kh in range(KV):
        for g in range(GROUP):
            h = kh * GROUP + g
            piece = q_ref[:, h * HEAD : (h + 1) * HEAD].astype(F32)
            cols = slice(g * TOK, (g + 1) * TOK)
            whole = jnp.concatenate([piece, jnp.broadcast_to(closed, (TOK, 128))], axis=1)
            if g % 2 == 0:
                held = whole
            else:
                two = jnp.concatenate([held, whole], axis=0)
                qx[kh, :, (g - 1) * TOK : (g + 1) * TOK] = two.T.astype(BF)
        sc = dot(kv[0:TOK, kh * HEAD : (kh + 1) * HEAD], qx[kh, 0:128, :])
        sc = jnp.where(tri, sc, VERY_LOW)
        top = jnp.max(sc, axis=0, keepdims=True)
        w = jnp.exp2((sc - top) * SCORE)
        m_p[kh] = top
        l_p[kh] = jnp.sum(w, axis=0, keepdims=True)
        vt = kv[0:TOK, 256 + kh * HEAD : 256 + (kh + 1) * HEAD].astype(F32).T.astype(BF)
        o_p[kh] = dot(vt, w.astype(BF))

    for h in range(KV * GROUP):
        for t in range(STEPS):
            dq_s[h * 8 + t * ROWS : h * 8 + (t + 1) * ROWS, :] = dq_ref[
                t, :, h * HEAD : (h + 1) * HEAD
            ].astype(F32)
    nk_s[...] = jnp.zeros_like(nk_s)
    nv_s[...] = jnp.zeros_like(nv_s)
    for t in range(STEPS):
        nk_s[t * ROWS : (t + 1) * ROWS, :] = nk_ref[t].astype(F32)
        nv_s[t * ROWS : (t + 1) * ROWS, :] = nv_ref[t].astype(F32)
    dq = dq_s[...]
    turned = dot(dq.astype(BF), h2[0:128, 0:128])
    which = lax.broadcasted_iota(jnp.int32, (128, 1), 0) < 64
    turned = (turned * jnp.where(which, backward[0], backward[1])).T
    high = turned.astype(BF).astype(F32)
    low = turned - high
    zero = jnp.zeros((128, 128), F32)
    for part, a in enumerate((high, low)):
        cols = slice(part * 128, (part + 1) * 128)
        qd[0:128, cols] = jnp.where(first_head, a, zero).astype(BF)
        qd[128:256, cols] = jnp.where(first_head, zero, a).astype(BF)
    dqt = dq.T
    upper = jnp.where(first_head, dqt, zero).astype(BF)
    lower = jnp.where(first_head, zero, dqt).astype(BF)
    nk = nk_s[...].astype(BF)
    sc = dot(nk[:, 0:128], upper) + dot(nk[:, 128:256], lower)
    key_i = lax.broadcasted_iota(jnp.int32, (128, 128), 0)
    qry_i = lax.broadcasted_iota(jnp.int32, (128, 128), 1) % (STEPS * ROWS)
    seen = (
        (key_i < STEPS * ROWS)
        & (key_i % ROWS == qry_i % ROWS)
        & (key_i // ROWS <= qry_i // ROWS)
    )
    sc = jnp.where(seen, sc, VERY_LOW)
    top = jnp.max(sc, axis=0, keepdims=True)
    w = jnp.where(seen, jnp.exp2((sc - top) * SCORE), 0.0)
    m_d[...] = top
    m_0[...] = top
    l_d[...] = jnp.sum(w, axis=0, keepdims=True)
    nvt = nv_s[...].T.astype(BF)
    wide = dot(nvt, w.astype(BF))
    o_0[...] = jnp.where(first_head, wide[0:128], wide[128:256])
    o_d[...] = jnp.zeros_like(o_d)

    rows_in = lax.broadcasted_iota(jnp.int32, (HALF, 128), 0)
    lanes_in = lax.broadcasted_iota(jnp.int32, (HALF, 128), 1)
    part_y = [at((yh + o) % 2, 0, 0, 0) for o in (0, 1)]
    part_x = [at(0, (x + o) % XS, 0, 0) for o in range(XS)]
    part_z = [at(0, 0, (z + o) % ZS, 0) for o in range(ZS)]
    part_core = [(core + o) % 2 for o in (0, 1)]

    def compute(e, tile):
        first = e * OWN + tile * TILE
        for u in range(TILE // HALF):
            side, path, dx, dz = SOURCES[tile * (TILE // HALF) + u]
            block = part_y[side] + part_x[dx % XS] + part_z[dz % ZS] + part_core[e]
            here = slice(u * HALF, (u + 1) * HALF)
            oh[here, :] = jnp.where(lanes_in == block, 1.0, 0.0).astype(BF)
            pos[here, :] = rows_in + (block * TOK + path * HALF)

        keys = kv[pl.ds(first, TILE), 0:256]
        blocks = oh[...]
        scores = [
            dot(
                jnp.concatenate([keys[:, kh * HEAD : (kh + 1) * HEAD], blocks], axis=1), qx[kh]
            )
            for kh in range(KV)
        ]
        vals_t = kv[pl.ds(first, TILE), 256:512].T

        def code(rot, axis):
            return jnp.concatenate(
                [
                    jnp.clip(
                        jnp.floor(lax.slice_in_dim(rot, j * HEAD, (j + 1) * HEAD, axis=axis) * forward[j] + 0.5),
                        -level[j],
                        level[j],
                    ).astype(BF)
                    for j in range(KV)
                ],
                axis=axis,
            )

        coded_k = code(dot(keys, h2[...]), 1)
        coded_v = code(dot(h2[...], vals_t), 0)
        two = dot(coded_k, qd[...])
        for kh in range(KV):
            sc = scores[kh]
            old = m_p[kh]
            top = jnp.maximum(old, jnp.max(sc, axis=0, keepdims=True))
            w = jnp.exp2(sc * SCORE - top * SCORE)
            fade = jnp.exp2((old - top) * SCORE)
            m_p[kh] = top
            l_p[kh] = l_p[kh] * fade + jnp.sum(w, axis=0, keepdims=True)
            o_p[kh] = o_p[kh] * fade + dot(vals_t[kh * HEAD : (kh + 1) * HEAD, :], w.astype(BF))
        sc = jnp.where(pos[...] < limits, two[:, 0:128] + two[:, 128:256], VERY_LOW)
        old = m_d[...]
        top = jnp.maximum(old, jnp.max(sc, axis=0, keepdims=True))
        w = jnp.exp2(sc * SCORE - top * SCORE)
        fade = jnp.exp2((old - top) * SCORE)
        m_d[...] = top
        l_d[...] = l_d[...] * fade + jnp.sum(w, axis=0, keepdims=True)
        o_d[...] = o_d[...] * fade + dot(coded_v, w.astype(BF))


    shared = 0
    for k, (_, tiles) in enumerate(PLAN):
        if k > 1:
            wave_copy(k).wait_recv()
            forwards(k)
            to_sibling(k).start()
        for e, t in tiles:
            while e == 1 and shared <= NEED[t]:
                to_sibling(shared).wait_recv()
                shared += 1
            compute(e, t)

    turned = jnp.where(first_head, o_d[0:128, :], o_d[128:256, :])
    high = turned.astype(BF)
    low = (turned - high.astype(F32)).astype(BF)
    sign = h2[0:128, 0:128]
    plain = (dot(sign, high) + dot(sign, low)) * jnp.where(first_head, backward[0], backward[1])
    plain = plain + o_0[...] * jnp.exp2((m_0[...] - m_d[...]) * SCORE)
    dattn[...] = (plain / l_d[...]).T
    total = jnp.zeros((8, 128), F32)
    for h in range(KV * GROUP):
        a = dattn[h * 8 : (h + 1) * 8, :]
        total = total + a * a
    sq_mine[TOK : TOK + 8, :] = jnp.broadcast_to(jnp.sum(total, axis=1, keepdims=True), (8, 128))

    total = jnp.zeros((TOK, 128), F32)
    for kh in range(KV):
        done = (o_p[kh] / l_p[kh]).T
        attn[kh] = done
        for g in range(GROUP):
            a = done[g * TOK : (g + 1) * TOK, :]
            total = total + a * a
    sq_mine[0:TOK, :] = jnp.broadcast_to(jnp.sum(total, axis=1, keepdims=True), (TOK, 128))
    swap = pltpu.make_async_remote_copy(
        src_ref=sq_mine,
        dst_ref=sq_theirs,
        send_sem=g_send,
        recv_sem=g_recv,
        device_id=(s, 1 - grp),
        device_id_type=MESH,
    )
    swap.start()

    for c in ycopies:
        c.wait_send()
    for k in range(NW):
        if ORDER[k][0] > 0:
            wave_copy(k).wait_send()
        to_sibling(k).wait_send()
    swap.wait()
    norm = lax.rsqrt((sq_mine[...] + sq_theirs[...]) / WIDE + EPS)
    for kh in range(KV):
        for g in range(GROUP):
            h = kh * GROUP + g
            out_ref[:, h * HEAD : (h + 1) * HEAD] = (
                attn[kh, g * TOK : (g + 1) * TOK, :] * norm[0:TOK]
            ).astype(BF)
            a = (dattn[h * 8 : (h + 1) * 8, :] * norm[TOK : TOK + 8]).astype(BF)
            for t in range(STEPS):
                dout_ref[t, :, h * HEAD : (h + 1) * HEAD] = a[t * ROWS : (t + 1) * ROWS, :]


def local(q, k, v, mask, widths, exps, dq, nk, nv, ctx):
    vmem = pl.BlockSpec(memory_space=pltpu.VMEM)
    hbm = pl.BlockSpec(memory_space=pltpu.HBM)
    dma = pltpu.SemaphoreType.DMA
    return pl.pallas_call(
        kernel,
        out_shape=(
            jax.ShapeDtypeStruct(q.shape, BF),
            jax.ShapeDtypeStruct(dq.shape, BF),
        ),
        in_specs=[hbm] * 10,
        out_specs=(vmem, vmem),
        scratch_shapes=[
            pltpu.SMEM((KV,), jnp.int32),
            pltpu.SMEM((KV,), jnp.int32),
            pltpu.SMEM((ROWS,), jnp.int32),
            pltpu.VMEM(q.shape, BF),
            pltpu.VMEM(mask.shape, jnp.int32),
            pltpu.VMEM(dq.shape, BF),
            pltpu.VMEM(nk.shape, BF),
            pltpu.VMEM(nv.shape, BF),
            pltpu.VMEM((2 * OWN, 512), BF),
            pltpu.VMEM((KV, 256, 512), BF),
            pltpu.VMEM((256, 256), BF),
            pltpu.VMEM((256, 256), BF),
            pltpu.VMEM((TILE, 128), BF),
            pltpu.VMEM((TILE, 128), jnp.int32),
            pltpu.VMEM((KV, 1, 512), F32),
            pltpu.VMEM((KV, 1, 512), F32),
            pltpu.VMEM((KV, 128, 512), F32),
            pltpu.VMEM((1, 128), F32),
            pltpu.VMEM((1, 128), F32),
            pltpu.VMEM((256, 128), F32),
            pltpu.VMEM((1, 128), F32),
            pltpu.VMEM((128, 128), F32),
            pltpu.VMEM((128, 128), F32),
            pltpu.VMEM((128, 256), F32),
            pltpu.VMEM((128, 256), F32),
            pltpu.VMEM((KV, 512, 128), F32),
            pltpu.VMEM((128, 128), F32),
            pltpu.VMEM((TOK + 8, 128), F32),
            pltpu.VMEM((TOK + 8, 128), F32),
            dma((10,)),
            dma((2,)),
            dma((NW,)),
            dma((NW,)),
            dma((NW,)),
            dma((NW,)),
            dma,
            dma,
        ],
        compiler_params=pltpu.CompilerParams(
            collective_id=0, has_side_effects=True, vmem_limit_bytes=67_043_328
        ),
    )(q, k, v, mask, widths, exps, dq, nk, nv, ctx)


def solution(mesh):
    placed = (
        P("seq", "grp"),
        P("seq", "grp"),
        P("seq", "grp"),
        P(),
        P("grp"),
        P("grp"),
        P(None, "seq", "grp"),
        P(None, "seq", "grp"),
        P(None, "seq", "grp"),
        P("seq"),
    )
    return jax.shard_map(
        local,
        mesh=mesh,
        in_specs=placed,
        out_specs=(P("seq", "grp"), P(None, "seq", "grp")),
        check_vma=False,
    )
```

```python
import math

import jax
import jax.numpy as jnp
from jax import lax
from jax.experimental import pallas as pl
from jax.experimental.pallas import tpu as pltpu
from jax.sharding import PartitionSpec as P

HEADS = 32
KV = 2
GROUP = 8
HEAD = 128
STEPS = 4
TOK = 64
ROWS = 2
XS, ZS = 4, 8
HALF = TOK // 2
TILE = 512
VERY_LOW = -1e30
EPS = 1e-6
WIDE = HEADS * HEAD
SCORE = math.log2(math.e) / math.sqrt(HEAD)

BF = jnp.bfloat16
F32 = jnp.float32
MESH = pl.DeviceIdType.MESH

PLAN = [
    ((0, 0, 0), []),
    ((0, 0, 1), []),
    ((1, 0, 0), []),
    ((1, 0, 1), []),
    ((0, 1, 0), []),
    ((0, 1, 1), []),
    ((1, 1, 0), []),
    ((2, 0, 0), [(0, 0)]),
    ((1, 1, 1), []),
    ((2, 0, 1), [(0, 1), (1, 0), (1, 1)]),
    ((2, 1, 0), []),
    ((2, 1, 1), []),
    ((3, 0, 0), [(0, 2)]),
    ((3, 0, 1), [(0, 3), (1, 2)]),
    ((3, 1, 0), [(1, 3)]),
    ((3, 1, 1), [(0, 4)]),
    ((4, 0, 0), []),
    ((4, 0, 1), [(1, 4)]),
    ((4, 1, 0), [(0, 5)]),
    ((4, 1, 1), []),
    ((5, 0, 0), [(1, 5), (0, 6), (1, 6)]),
    ((5, 1, 0), []),
    ((6, 0, 1), []),
    ((5, 0, 1), []),
    ((6, 0, 0), []),
    ((6, 1, 1), []),
    ((6, 1, 0), []),
    ((5, 1, 1), [(0, 7), (1, 7)]),
]
ORDER = [g for g, _ in PLAN]
NW = len(ORDER)
OFFSETS = [(dx, dz) for dx in (0, -1, 1, 2) for dz in (0, -1, 1, -2, 2, -3, 3, 4)]


def sort_key(path, side):
    far = -9 if side == 0 else 9

    def key(off):
        dx, dz = off
        kx = far if dx == 2 else dx
        kz = far if dz == 4 else dz
        return (kz, kx) if path == 0 else (kx, kz)

    return key


UNITS = []
SLOT = {}
START = []
for d, side, path in ORDER:
    START.append(len(SLOT) * HALF)
    UNITS.append(
        sorted((o for o in OFFSETS if abs(o[0]) + abs(o[1]) == d), key=sort_key(path, side))
    )
    for off in UNITS[-1]:
        SLOT[(side, path, *off)] = len(SLOT)
START.append(len(SLOT) * HALF)
SOURCES = list(SLOT)
OWN = START[-1]
NTILE = OWN // TILE
NEED = [max(k for k in range(NW) if START[k] < (t + 1) * TILE) for t in range(NTILE)]
WAVE = {u: k for k in range(NW) for u in range(START[k], START[k + 1], HALF)}
LAST = (2, 4)


def hops(n, far, side):
    if n == 0:
        return [(1, -1), (-1, 1)]
    if n == far:
        return []
    way = 1 if n < 0 else -1
    if abs(n) == far - 1:
        return [(way, far)] if (way == 1) == (side == 0) else []
    return [(way, n - way)]


def messages(k):
    _, side, path = ORDER[k]
    out = []
    for dx, dz in UNITS[k]:
        here = SLOT[(side, path, dx, dz)] * HALF
        steps = []
        if path == 0 or dx == 0:
            steps += [("z", way, (dx, n)) for way, n in hops(dz, 4, side)]
        if path == 1 or dz == 0:
            steps += [("x", way, (n, dz)) for way, n in hops(dx, 2, side)]
        steps = [m for m in steps if m[2] != LAST]
        way = 1 if side == 0 else -1
        if path == 0 and (dx, dz) == (2, -2 * way):
            steps.append(("z", 2 * way, LAST))
        if path == 1 and (dx, dz) == (0, 4):
            steps.append(("x", 2 * way, LAST))
        for axis, way, there in steps:
            out.append((path, axis, way, here, SLOT[(side, path, *there)] * HALF))
    out.sort(key=lambda m: (m[0], m[1], m[2], m[3]))
    merged = []
    for path, axis, way, here, there in out:
        if merged:
            p, a, w, h, t, n = merged[-1]
            if (p, a, w) == (path, axis, way) and h + n == here and t + n == there:
                merged[-1] = (p, a, w, h, t, n + HALF)
                continue
        merged.append((path, axis, way, here, there, HALF))
    merged.sort(key=lambda m: m[0] if m[1] == "z" else 1 - m[0])
    return [m[1:] for m in merged]


def dot(a, b):
    return jnp.dot(a, b, preferred_element_type=F32)


def choose(n, first, values):
    out = jnp.float32(values[0])
    for i, v in enumerate(values[1:]):
        out = jnp.where(n == first + 1 + i, jnp.float32(v), out)
    return out


def kernel(
    q_hbm,
    k_hbm,
    v_hbm,
    mask_hbm,
    widths_hbm,
    exps_hbm,
    dq_hbm,
    nk_hbm,
    nv_hbm,
    ctx_hbm,
    out_ref,
    dout_ref,
    widths,
    exps,
    ctx,
    q_ref,
    mask_ref,
    dq_ref,
    nk_ref,
    nv_ref,
    kv,
    qx,
    qd,
    h2,
    oh,
    pos,
    m_p,
    l_p,
    o_p,
    m_d,
    l_d,
    o_d,
    m_0,
    o_0,
    dq_s,
    nk_s,
    nv_s,
    attn,
    dattn,
    sq_mine,
    sq_theirs,
    load_sem,
    y_send,
    send_sem,
    recv_sem,
    sib_send,
    sib_recv,
    g_send,
    g_recv,
):
    s = lax.axis_index("seq")
    grp = lax.axis_index("grp")
    core = s % 2
    z = (s // 2) % ZS
    x = (s // (2 * ZS)) % XS
    yh = s // (2 * ZS * XS)

    def at(yh_, x_, z_, core_):
        return ((yh_ * XS + x_) * ZS + z_) * 2 + core_

    peers = {
        ("x", 1): at(yh, (x + 1) % XS, z, core),
        ("x", -1): at(yh, (x + XS - 1) % XS, z, core),
        ("z", 1): at(yh, x, (z + 1) % ZS, core),
        ("z", -1): at(yh, x, (z + ZS - 1) % ZS, core),
        ("x", 2): at(yh, (x + 2) % XS, z, core),
        ("z", 2): at(yh, x, (z + 2) % ZS, core),
        ("z", -2): at(yh, x, (z + ZS - 2) % ZS, core),
    }
    greeted = list(peers.values())
    peers["x", -2] = peers["x", 2]
    across = at(1 - yh, x, z, core)
    sibling = at(yh, x, z, 1 - core)

    barrier = pltpu.get_barrier_semaphore()
    for dev in (*greeted, across, sibling):
        pl.semaphore_signal(barrier, inc=1, device_id=(dev, grp), device_id_type=MESH)
    pl.semaphore_signal(barrier, inc=1, device_id=(s, 1 - grp), device_id_type=MESH)

    loads = [
        pltpu.make_async_copy(src, dst, load_sem.at[i])
        for i, (src, dst) in enumerate(
            (
                (k_hbm, kv.at[pl.ds(0, TOK), pl.ds(0, 256)]),
                (v_hbm, kv.at[pl.ds(0, TOK), pl.ds(256, 256)]),
                (q_hbm, q_ref),
                (mask_hbm, mask_ref),
                (widths_hbm, widths),
                (exps_hbm, exps),
                (ctx_hbm, ctx),
                (dq_hbm, dq_ref),
                (nk_hbm, nk_ref),
                (nv_hbm, nv_ref),
            )
        )
    ]
    for c in loads:
        c.start()

    def remote(src_row, dst_row, count, ssem, rsem, dev):
        return pltpu.make_async_remote_copy(
            src_ref=kv.at[pl.ds(src_row, count), :],
            dst_ref=kv.at[pl.ds(dst_row, count), :],
            send_sem=ssem,
            recv_sem=rsem,
            device_id=(dev, grp),
            device_id_type=MESH,
        )

    def forwards(k):
        for axis, way, here, there, count in messages(k):
            n = WAVE[there]
            remote(
                here, there, count, send_sem.at[n], recv_sem.at[n], peers[(axis, way)]
            ).start()

    def wave_copy(k):
        return remote(
            START[k], START[k], START[k + 1] - START[k], send_sem.at[k], recv_sem.at[k], sibling
        )

    def to_sibling(k):
        return remote(
            START[k],
            OWN + START[k],
            START[k + 1] - START[k],
            sib_send.at[k],
            sib_recv.at[k],
            sibling,
        )

    theirs = [ORDER.index((0, 1, path)) for path in (0, 1)]
    ycopies = [
        remote(path * HALF, START[k], HALF, y_send.at[path], recv_sem.at[k], across)
        for path, k in enumerate(theirs)
    ]
    loads[0].wait()
    loads[1].wait()
    pl.semaphore_wait(barrier, len(greeted) + 3)
    for c in ycopies:
        c.start()
    for k in (0, 1):
        forwards(k)
        to_sibling(k).start()
    for c in loads[2:]:
        c.wait()

    i0 = lax.broadcasted_iota(jnp.int32, (256, 256), 0)
    i1 = lax.broadcasted_iota(jnp.int32, (256, 256), 1)
    both = (i0 & i1) & 127
    parity = jnp.zeros((256, 256), jnp.int32)
    for b in range(7):
        parity = parity + ((both >> b) & 1)
    sign = (1 - 2 * (parity % 2)).astype(F32)
    h2[...] = jnp.where((i0 // 128) == (i1 // 128), sign, 0.0).astype(BF)

    lane = lax.broadcasted_iota(jnp.int32, (1, 128), 1)
    first_head = lane < 64
    level = [choose(widths[i], 3, [3.0, 7.0, 15.0, 31.0, 63.0, 127.0]) for i in range(KV)]
    power = [choose(exps[i], 1, [2.0, 4.0, 8.0, 16.0]) for i in range(KV)]
    inverse = [choose(exps[i], 1, [0.5, 0.25, 0.125, 0.0625]) for i in range(KV)]
    forward = [p / math.sqrt(HEAD) for p in power]
    backward = [p / math.sqrt(HEAD) for p in inverse]
    limits = jnp.where(lane % 2 == 0, ctx[0], ctx[1])

    row = mask_ref[pl.ds(s, 1), :]
    closed = jnp.where((row == 1) & (lane < s), 0.0, VERY_LOW).astype(F32)
    tri = lax.broadcasted_iota(jnp.int32, (TOK, 512), 0) <= (
        lax.broadcasted_iota(jnp.int32, (TOK, 512), 1) % TOK
    )
    for kh in range(KV):
        for g in range(GROUP):
            h = kh * GROUP + g
            piece = q_ref[:, h * HEAD : (h + 1) * HEAD].astype(F32)
            cols = slice(g * TOK, (g + 1) * TOK)
            whole = jnp.concatenate([piece, jnp.broadcast_to(closed, (TOK, 128))], axis=1)
            if g % 2 == 0:
                held = whole
            else:
                two = jnp.concatenate([held, whole], axis=0)
                qx[kh, :, (g - 1) * TOK : (g + 1) * TOK] = two.T.astype(BF)
        sc = dot(kv[0:TOK, kh * HEAD : (kh + 1) * HEAD], qx[kh, 0:128, :])
        sc = jnp.where(tri, sc, VERY_LOW)
        top = jnp.max(sc, axis=0, keepdims=True)
        w = jnp.exp2((sc - top) * SCORE)
        m_p[kh] = top
        l_p[kh] = jnp.sum(w, axis=0, keepdims=True)
        vt = kv[0:TOK, 256 + kh * HEAD : 256 + (kh + 1) * HEAD].astype(F32).T.astype(BF)
        o_p[kh] = dot(vt, w.astype(BF))

    for h in range(KV * GROUP):
        for t in range(STEPS):
            dq_s[h * 8 + t * ROWS : h * 8 + (t + 1) * ROWS, :] = dq_ref[
                t, :, h * HEAD : (h + 1) * HEAD
            ].astype(F32)
    nk_s[...] = jnp.zeros_like(nk_s)
    nv_s[...] = jnp.zeros_like(nv_s)
    for t in range(STEPS):
        nk_s[t * ROWS : (t + 1) * ROWS, :] = nk_ref[t].astype(F32)
        nv_s[t * ROWS : (t + 1) * ROWS, :] = nv_ref[t].astype(F32)
    dq = dq_s[...]
    turned = dot(dq.astype(BF), h2[0:128, 0:128])
    which = lax.broadcasted_iota(jnp.int32, (128, 1), 0) < 64
    turned = (turned * jnp.where(which, backward[0], backward[1])).T
    high = turned.astype(BF).astype(F32)
    low = turned - high
    zero = jnp.zeros((128, 128), F32)
    for part, a in enumerate((high, low)):
        cols = slice(part * 128, (part + 1) * 128)
        qd[0:128, cols] = jnp.where(first_head, a, zero).astype(BF)
        qd[128:256, cols] = jnp.where(first_head, zero, a).astype(BF)
    dqt = dq.T
    upper = jnp.where(first_head, dqt, zero).astype(BF)
    lower = jnp.where(first_head, zero, dqt).astype(BF)
    nk = nk_s[...].astype(BF)
    sc = dot(nk[:, 0:128], upper) + dot(nk[:, 128:256], lower)
    key_i = lax.broadcasted_iota(jnp.int32, (128, 128), 0)
    qry_i = lax.broadcasted_iota(jnp.int32, (128, 128), 1) % (STEPS * ROWS)
    seen = (
        (key_i < STEPS * ROWS)
        & (key_i % ROWS == qry_i % ROWS)
        & (key_i // ROWS <= qry_i // ROWS)
    )
    sc = jnp.where(seen, sc, VERY_LOW)
    top = jnp.max(sc, axis=0, keepdims=True)
    w = jnp.where(seen, jnp.exp2((sc - top) * SCORE), 0.0)
    m_d[...] = top
    m_0[...] = top
    l_d[...] = jnp.sum(w, axis=0, keepdims=True)
    nvt = nv_s[...].T.astype(BF)
    wide = dot(nvt, w.astype(BF))
    o_0[...] = jnp.where(first_head, wide[0:128], wide[128:256])
    o_d[...] = jnp.zeros_like(o_d)

    rows_in = lax.broadcasted_iota(jnp.int32, (HALF, 128), 0)
    lanes_in = lax.broadcasted_iota(jnp.int32, (HALF, 128), 1)
    part_y = [at((yh + o) % 2, 0, 0, 0) for o in (0, 1)]
    part_x = [at(0, (x + o) % XS, 0, 0) for o in range(XS)]
    part_z = [at(0, 0, (z + o) % ZS, 0) for o in range(ZS)]
    part_core = [(core + o) % 2 for o in (0, 1)]

    def compute(e, tile):
        first = e * OWN + tile * TILE
        for u in range(TILE // HALF):
            side, path, dx, dz = SOURCES[tile * (TILE // HALF) + u]
            block = part_y[side] + part_x[dx % XS] + part_z[dz % ZS] + part_core[e]
            here = slice(u * HALF, (u + 1) * HALF)
            oh[here, :] = jnp.where(lanes_in == block, 1.0, 0.0).astype(BF)
            pos[here, :] = rows_in + (block * TOK + path * HALF)

        keys = kv[pl.ds(first, TILE), 0:256]
        blocks = oh[...]
        scores = [
            dot(
                jnp.concatenate([keys[:, kh * HEAD : (kh + 1) * HEAD], blocks], axis=1), qx[kh]
            )
            for kh in range(KV)
        ]
        vals_t = kv[pl.ds(first, TILE), 256:512].T

        def code(rot, axis):
            return jnp.concatenate(
                [
                    jnp.clip(
                        jnp.floor(lax.slice_in_dim(rot, j * HEAD, (j + 1) * HEAD, axis=axis) * forward[j] + 0.5),
                        -level[j],
                        level[j],
                    ).astype(BF)
                    for j in range(KV)
                ],
                axis=axis,
            )

        coded_k = code(dot(keys, h2[...]), 1)
        coded_v = code(dot(h2[...], vals_t), 0)
        two = dot(coded_k, qd[...])
        for kh in range(KV):
            sc = scores[kh]
            old = m_p[kh]
            top = jnp.maximum(old, jnp.max(sc, axis=0, keepdims=True))
            w = jnp.exp2(sc * SCORE - top * SCORE)
            fade = jnp.exp2((old - top) * SCORE)
            m_p[kh] = top
            l_p[kh] = l_p[kh] * fade + jnp.sum(w, axis=0, keepdims=True)
            o_p[kh] = o_p[kh] * fade + dot(vals_t[kh * HEAD : (kh + 1) * HEAD, :], w.astype(BF))
        sc = jnp.where(pos[...] < limits, two[:, 0:128] + two[:, 128:256], VERY_LOW)
        old = m_d[...]
        top = jnp.maximum(old, jnp.max(sc, axis=0, keepdims=True))
        w = jnp.exp2(sc * SCORE - top * SCORE)
        fade = jnp.exp2((old - top) * SCORE)
        m_d[...] = top
        l_d[...] = l_d[...] * fade + jnp.sum(w, axis=0, keepdims=True)
        o_d[...] = o_d[...] * fade + dot(coded_v, w.astype(BF))


    shared = 0
    for k, (_, tiles) in enumerate(PLAN):
        if k > 1:
            wave_copy(k).wait_recv()
            forwards(k)
            to_sibling(k).start()
        for e, t in tiles:
            while e == 1 and shared <= NEED[t]:
                to_sibling(shared).wait_recv()
                shared += 1
            compute(e, t)

    turned = jnp.where(first_head, o_d[0:128, :], o_d[128:256, :])
    high = turned.astype(BF)
    low = (turned - high.astype(F32)).astype(BF)
    sign = h2[0:128, 0:128]
    plain = (dot(sign, high) + dot(sign, low)) * jnp.where(first_head, backward[0], backward[1])
    plain = plain + o_0[...] * jnp.exp2((m_0[...] - m_d[...]) * SCORE)
    dattn[...] = (plain / l_d[...]).T
    total = jnp.zeros((8, 128), F32)
    for h in range(KV * GROUP):
        a = dattn[h * 8 : (h + 1) * 8, :]
        total = total + a * a
    sq_mine[TOK : TOK + 8, :] = jnp.broadcast_to(jnp.sum(total, axis=1, keepdims=True), (8, 128))

    total = jnp.zeros((TOK, 128), F32)
    for kh in range(KV):
        done = (o_p[kh] / l_p[kh]).T
        attn[kh] = done
        for g in range(GROUP):
            a = done[g * TOK : (g + 1) * TOK, :]
            total = total + a * a
    sq_mine[0:TOK, :] = jnp.broadcast_to(jnp.sum(total, axis=1, keepdims=True), (TOK, 128))
    swap = pltpu.make_async_remote_copy(
        src_ref=sq_mine,
        dst_ref=sq_theirs,
        send_sem=g_send,
        recv_sem=g_recv,
        device_id=(s, 1 - grp),
        device_id_type=MESH,
    )
    swap.start()

    for c in ycopies:
        c.wait_send()
    for k in range(NW):
        if ORDER[k][0] > 0:
            wave_copy(k).wait_send()
        to_sibling(k).wait_send()
    swap.wait()
    norm = lax.rsqrt((sq_mine[...] + sq_theirs[...]) / WIDE + EPS)
    for kh in range(KV):
        for g in range(GROUP):
            h = kh * GROUP + g
            out_ref[:, h * HEAD : (h + 1) * HEAD] = (
                attn[kh, g * TOK : (g + 1) * TOK, :] * norm[0:TOK]
            ).astype(BF)
            a = (dattn[h * 8 : (h + 1) * 8, :] * norm[TOK : TOK + 8]).astype(BF)
            for t in range(STEPS):
                dout_ref[t, :, h * HEAD : (h + 1) * HEAD] = a[t * ROWS : (t + 1) * ROWS, :]


def local(q, k, v, mask, widths, exps, dq, nk, nv, ctx):
    vmem = pl.BlockSpec(memory_space=pltpu.VMEM)
    hbm = pl.BlockSpec(memory_space=pltpu.HBM)
    dma = pltpu.SemaphoreType.DMA
    return pl.pallas_call(
        kernel,
        out_shape=(
            jax.ShapeDtypeStruct(q.shape, BF),
            jax.ShapeDtypeStruct(dq.shape, BF),
        ),
        in_specs=[hbm] * 10,
        out_specs=(vmem, vmem),
        scratch_shapes=[
            pltpu.SMEM((KV,), jnp.int32),
            pltpu.SMEM((KV,), jnp.int32),
            pltpu.SMEM((ROWS,), jnp.int32),
            pltpu.VMEM(q.shape, BF),
            pltpu.VMEM(mask.shape, jnp.int32),
            pltpu.VMEM(dq.shape, BF),
            pltpu.VMEM(nk.shape, BF),
            pltpu.VMEM(nv.shape, BF),
            pltpu.VMEM((2 * OWN, 512), BF),
            pltpu.VMEM((KV, 256, 512), BF),
            pltpu.VMEM((256, 256), BF),
            pltpu.VMEM((256, 256), BF),
            pltpu.VMEM((TILE, 128), BF),
            pltpu.VMEM((TILE, 128), jnp.int32),
            pltpu.VMEM((KV, 1, 512), F32),
            pltpu.VMEM((KV, 1, 512), F32),
            pltpu.VMEM((KV, 128, 512), F32),
            pltpu.VMEM((1, 128), F32),
            pltpu.VMEM((1, 128), F32),
            pltpu.VMEM((256, 128), F32),
            pltpu.VMEM((1, 128), F32),
            pltpu.VMEM((128, 128), F32),
            pltpu.VMEM((128, 128), F32),
            pltpu.VMEM((128, 256), F32),
            pltpu.VMEM((128, 256), F32),
            pltpu.VMEM((KV, 512, 128), F32),
            pltpu.VMEM((128, 128), F32),
            pltpu.VMEM((TOK + 8, 128), F32),
            pltpu.VMEM((TOK + 8, 128), F32),
            dma((10,)),
            dma((2,)),
            dma((NW,)),
            dma((NW,)),
            dma((NW,)),
            dma((NW,)),
            dma,
            dma,
        ],
        compiler_params=pltpu.CompilerParams(
            collective_id=0, has_side_effects=True, vmem_limit_bytes=67_043_328
        ),
    )(q, k, v, mask, widths, exps, dq, nk, nv, ctx)


def solution(mesh):
    placed = (
        P("seq", "grp"),
        P("seq", "grp"),
        P("seq", "grp"),
        P(),
        P("grp"),
        P("grp"),
        P(None, "seq", "grp"),
        P(None, "seq", "grp"),
        P(None, "seq", "grp"),
        P("seq"),
    )
    return jax.shard_map(
        local,
        mesh=mesh,
        in_specs=placed,
        out_specs=(P("seq", "grp"), P(None, "seq", "grp")),
        check_vma=False,
    )
```

```python
import math

import jax
import jax.numpy as jnp
from jax import lax
from jax.experimental import pallas as pl
from jax.experimental.pallas import tpu as pltpu
from jax.sharding import PartitionSpec as P

HEADS = 32
KV = 2
GROUP = 8
HEAD = 128
STEPS = 4
TOK = 64
ROWS = 2
XS, ZS = 4, 8
HALF = TOK // 2
TILE = 512
VERY_LOW = -1e30
EPS = 1e-6
WIDE = HEADS * HEAD
SCORE = math.log2(math.e) / math.sqrt(HEAD)

BF = jnp.bfloat16
F32 = jnp.float32
MESH = pl.DeviceIdType.MESH

PLAN = [
    ((0, 0, 0), []),
    ((0, 0, 1), []),
    ((1, 0, 0), []),
    ((1, 0, 1), []),
    ((0, 1, 0), []),
    ((0, 1, 1), []),
    ((1, 1, 0), []),
    ((2, 0, 0), [(0, 0)]),
    ((1, 1, 1), []),
    ((2, 0, 1), [(0, 1), (1, 0), (1, 1)]),
    ((2, 1, 0), []),
    ((2, 1, 1), []),
    ((3, 0, 0), [(0, 2)]),
    ((3, 0, 1), [(0, 3), (1, 2)]),
    ((3, 1, 0), [(1, 3)]),
    ((3, 1, 1), [(0, 4)]),
    ((4, 0, 0), []),
    ((4, 0, 1), [(1, 4)]),
    ((4, 1, 0), [(0, 5)]),
    ((4, 1, 1), []),
    ((5, 0, 0), [(1, 5), (0, 6), (1, 6)]),
    ((5, 1, 0), []),
    ((6, 0, 1), []),
    ((5, 0, 1), [(0, 7)]),
    ((6, 0, 0), []),
    ((6, 1, 1), []),
    ((6, 1, 0), []),
    ((5, 1, 1), [(1, 7), (0, 8), (1, 8)]),
]
ORDER = [g for g, _ in PLAN]
NW = len(ORDER)
OFFSETS = [(dx, dz) for dx in (0, -1, 1, 2) for dz in (0, -1, 1, -2, 2, -3, 3, 4)]


def sort_key(path, side):
    far = -9 if side == 0 else 9

    def key(off):
        dx, dz = off
        kx = far if dx == 2 else dx
        kz = far if dz == 4 else dz
        return (kz, kx) if path == 0 else (kx, kz)

    return key


UNITS = []
SLOT = {}
START = []
for d, side, path in ORDER:
    START.append(len(SLOT) * HALF)
    UNITS.append(
        sorted((o for o in OFFSETS if abs(o[0]) + abs(o[1]) == d), key=sort_key(path, side))
    )
    for off in UNITS[-1]:
        SLOT[(side, path, *off)] = len(SLOT)
START.append(len(SLOT) * HALF)
SOURCES = list(SLOT)
OWN = START[-1]
TILES = [(i * TILE, TILE) for i in range(OWN // TILE - 1)] + [(OWN - 512, 256), (OWN - 256, 256)]
NEED = [max(k for k in range(NW) if START[k] < t + n) for t, n in TILES]
WAVE = {u: k for k in range(NW) for u in range(START[k], START[k + 1], HALF)}
LAST = (2, 4)


def hops(n, far, side):
    if n == 0:
        return [(1, -1), (-1, 1)]
    if n == far:
        return []
    way = 1 if n < 0 else -1
    if abs(n) == far - 1:
        return [(way, far)] if (way == 1) == (side == 0) else []
    return [(way, n - way)]


def messages(k):
    _, side, path = ORDER[k]
    out = []
    for dx, dz in UNITS[k]:
        here = SLOT[(side, path, dx, dz)] * HALF
        steps = []
        if path == 0 or dx == 0:
            steps += [("z", way, (dx, n)) for way, n in hops(dz, 4, side)]
        if path == 1 or dz == 0:
            steps += [("x", way, (n, dz)) for way, n in hops(dx, 2, side)]
        steps = [m for m in steps if m[2] != LAST]
        way = 1 if side == 0 else -1
        if path == 0 and (dx, dz) == (2, -2 * way):
            steps.append(("z", 2 * way, LAST))
        if path == 1 and (dx, dz) == (0, 4):
            steps.append(("x", 2 * way, LAST))
        for axis, way, there in steps:
            out.append((path, axis, way, here, SLOT[(side, path, *there)] * HALF))
    out.sort(key=lambda m: (m[0], m[1], m[2], m[3]))
    merged = []
    for path, axis, way, here, there in out:
        if merged:
            p, a, w, h, t, n = merged[-1]
            if (p, a, w) == (path, axis, way) and h + n == here and t + n == there:
                merged[-1] = (p, a, w, h, t, n + HALF)
                continue
        merged.append((path, axis, way, here, there, HALF))
    merged.sort(key=lambda m: m[0] if m[1] == "z" else 1 - m[0])
    return [m[1:] for m in merged]


def dot(a, b):
    return jnp.dot(a, b, preferred_element_type=F32)


def choose(n, first, values):
    out = jnp.float32(values[0])
    for i, v in enumerate(values[1:]):
        out = jnp.where(n == first + 1 + i, jnp.float32(v), out)
    return out


def kernel(
    q_hbm,
    k_hbm,
    v_hbm,
    mask_hbm,
    widths_hbm,
    exps_hbm,
    dq_hbm,
    nk_hbm,
    nv_hbm,
    ctx_hbm,
    out_ref,
    dout_ref,
    widths,
    exps,
    ctx,
    q_ref,
    mask_ref,
    dq_ref,
    nk_ref,
    nv_ref,
    kv,
    qx,
    qd,
    h2,
    oh,
    pos,
    m_p,
    l_p,
    o_p,
    m_d,
    l_d,
    o_d,
    m_0,
    o_0,
    dq_s,
    nk_s,
    nv_s,
    attn,
    dattn,
    sq_mine,
    sq_theirs,
    load_sem,
    y_send,
    send_sem,
    recv_sem,
    sib_send,
    sib_recv,
    g_send,
    g_recv,
):
    s = lax.axis_index("seq")
    grp = lax.axis_index("grp")
    core = s % 2
    z = (s // 2) % ZS
    x = (s // (2 * ZS)) % XS
    yh = s // (2 * ZS * XS)

    def at(yh_, x_, z_, core_):
        return ((yh_ * XS + x_) * ZS + z_) * 2 + core_

    peers = {
        ("x", 1): at(yh, (x + 1) % XS, z, core),
        ("x", -1): at(yh, (x + XS - 1) % XS, z, core),
        ("z", 1): at(yh, x, (z + 1) % ZS, core),
        ("z", -1): at(yh, x, (z + ZS - 1) % ZS, core),
        ("x", 2): at(yh, (x + 2) % XS, z, core),
        ("z", 2): at(yh, x, (z + 2) % ZS, core),
        ("z", -2): at(yh, x, (z + ZS - 2) % ZS, core),
    }
    greeted = list(peers.values())
    peers["x", -2] = peers["x", 2]
    across = at(1 - yh, x, z, core)
    sibling = at(yh, x, z, 1 - core)

    barrier = pltpu.get_barrier_semaphore()
    for dev in (*greeted, across, sibling):
        pl.semaphore_signal(barrier, inc=1, device_id=(dev, grp), device_id_type=MESH)
    pl.semaphore_signal(barrier, inc=1, device_id=(s, 1 - grp), device_id_type=MESH)

    loads = [
        pltpu.make_async_copy(src, dst, load_sem.at[i])
        for i, (src, dst) in enumerate(
            (
                (k_hbm, kv.at[pl.ds(0, TOK), pl.ds(0, 256)]),
                (v_hbm, kv.at[pl.ds(0, TOK), pl.ds(256, 256)]),
                (q_hbm, q_ref),
                (mask_hbm, mask_ref),
                (widths_hbm, widths),
                (exps_hbm, exps),
                (ctx_hbm, ctx),
                (dq_hbm, dq_ref),
                (nk_hbm, nk_ref),
                (nv_hbm, nv_ref),
            )
        )
    ]
    for c in loads:
        c.start()

    def remote(src_row, dst_row, count, ssem, rsem, dev):
        return pltpu.make_async_remote_copy(
            src_ref=kv.at[pl.ds(src_row, count), :],
            dst_ref=kv.at[pl.ds(dst_row, count), :],
            send_sem=ssem,
            recv_sem=rsem,
            device_id=(dev, grp),
            device_id_type=MESH,
        )

    def forwards(k):
        for axis, way, here, there, count in messages(k):
            n = WAVE[there]
            remote(
                here, there, count, send_sem.at[n], recv_sem.at[n], peers[(axis, way)]
            ).start()

    def wave_copy(k):
        return remote(
            START[k], START[k], START[k + 1] - START[k], send_sem.at[k], recv_sem.at[k], sibling
        )

    def to_sibling(k):
        return remote(
            START[k],
            OWN + START[k],
            START[k + 1] - START[k],
            sib_send.at[k],
            sib_recv.at[k],
            sibling,
        )

    theirs = [ORDER.index((0, 1, path)) for path in (0, 1)]
    ycopies = [
        remote(path * HALF, START[k], HALF, y_send.at[path], recv_sem.at[k], across)
        for path, k in enumerate(theirs)
    ]
    loads[0].wait()
    loads[1].wait()
    pl.semaphore_wait(barrier, len(greeted) + 3)
    for c in ycopies:
        c.start()
    for k in (0, 1):
        forwards(k)
        to_sibling(k).start()
    for c in loads[2:]:
        c.wait()

    i0 = lax.broadcasted_iota(jnp.int32, (256, 256), 0)
    i1 = lax.broadcasted_iota(jnp.int32, (256, 256), 1)
    both = (i0 & i1) & 127
    parity = jnp.zeros((256, 256), jnp.int32)
    for b in range(7):
        parity = parity + ((both >> b) & 1)
    sign = (1 - 2 * (parity % 2)).astype(F32)
    h2[...] = jnp.where((i0 // 128) == (i1 // 128), sign, 0.0).astype(BF)

    lane = lax.broadcasted_iota(jnp.int32, (1, 128), 1)
    first_head = lane < 64
    level = [choose(widths[i], 3, [3.0, 7.0, 15.0, 31.0, 63.0, 127.0]) for i in range(KV)]
    power = [choose(exps[i], 1, [2.0, 4.0, 8.0, 16.0]) for i in range(KV)]
    inverse = [choose(exps[i], 1, [0.5, 0.25, 0.125, 0.0625]) for i in range(KV)]
    forward = [p / math.sqrt(HEAD) for p in power]
    backward = [p / math.sqrt(HEAD) for p in inverse]
    limits = jnp.where(lane % 2 == 0, ctx[0], ctx[1])

    row = mask_ref[pl.ds(s, 1), :]
    closed = jnp.where((row == 1) & (lane < s), 0.0, VERY_LOW).astype(F32)
    tri = lax.broadcasted_iota(jnp.int32, (TOK, 512), 0) <= (
        lax.broadcasted_iota(jnp.int32, (TOK, 512), 1) % TOK
    )
    for kh in range(KV):
        for g in range(GROUP):
            h = kh * GROUP + g
            piece = q_ref[:, h * HEAD : (h + 1) * HEAD].astype(F32)
            cols = slice(g * TOK, (g + 1) * TOK)
            whole = jnp.concatenate([piece, jnp.broadcast_to(closed, (TOK, 128))], axis=1)
            if g % 2 == 0:
                held = whole
            else:
                two = jnp.concatenate([held, whole], axis=0)
                qx[kh, :, (g - 1) * TOK : (g + 1) * TOK] = two.T.astype(BF)
        sc = dot(kv[0:TOK, kh * HEAD : (kh + 1) * HEAD], qx[kh, 0:128, :])
        sc = jnp.where(tri, sc, VERY_LOW)
        top = jnp.max(sc, axis=0, keepdims=True)
        w = jnp.exp2((sc - top) * SCORE)
        m_p[kh] = top
        l_p[kh] = jnp.sum(w, axis=0, keepdims=True)
        vt = kv[0:TOK, 256 + kh * HEAD : 256 + (kh + 1) * HEAD].astype(F32).T.astype(BF)
        o_p[kh] = dot(vt, w.astype(BF))

    for h in range(KV * GROUP):
        for t in range(STEPS):
            dq_s[h * 8 + t * ROWS : h * 8 + (t + 1) * ROWS, :] = dq_ref[
                t, :, h * HEAD : (h + 1) * HEAD
            ].astype(F32)
    nk_s[...] = jnp.zeros_like(nk_s)
    nv_s[...] = jnp.zeros_like(nv_s)
    for t in range(STEPS):
        nk_s[t * ROWS : (t + 1) * ROWS, :] = nk_ref[t].astype(F32)
        nv_s[t * ROWS : (t + 1) * ROWS, :] = nv_ref[t].astype(F32)
    dq = dq_s[...]
    turned = dot(dq.astype(BF), h2[0:128, 0:128])
    which = lax.broadcasted_iota(jnp.int32, (128, 1), 0) < 64
    turned = (turned * jnp.where(which, backward[0], backward[1])).T
    high = turned.astype(BF).astype(F32)
    low = turned - high
    zero = jnp.zeros((128, 128), F32)
    for part, a in enumerate((high, low)):
        cols = slice(part * 128, (part + 1) * 128)
        qd[0:128, cols] = jnp.where(first_head, a, zero).astype(BF)
        qd[128:256, cols] = jnp.where(first_head, zero, a).astype(BF)
    dqt = dq.T
    upper = jnp.where(first_head, dqt, zero).astype(BF)
    lower = jnp.where(first_head, zero, dqt).astype(BF)
    nk = nk_s[...].astype(BF)
    sc = dot(nk[:, 0:128], upper) + dot(nk[:, 128:256], lower)
    key_i = lax.broadcasted_iota(jnp.int32, (128, 128), 0)
    qry_i = lax.broadcasted_iota(jnp.int32, (128, 128), 1) % (STEPS * ROWS)
    seen = (
        (key_i < STEPS * ROWS)
        & (key_i % ROWS == qry_i % ROWS)
        & (key_i // ROWS <= qry_i // ROWS)
    )
    sc = jnp.where(seen, sc, VERY_LOW)
    top = jnp.max(sc, axis=0, keepdims=True)
    w = jnp.where(seen, jnp.exp2((sc - top) * SCORE), 0.0)
    m_d[...] = top
    m_0[...] = top
    l_d[...] = jnp.sum(w, axis=0, keepdims=True)
    nvt = nv_s[...].T.astype(BF)
    wide = dot(nvt, w.astype(BF))
    o_0[...] = jnp.where(first_head, wide[0:128], wide[128:256])
    o_d[...] = jnp.zeros_like(o_d)

    rows_in = lax.broadcasted_iota(jnp.int32, (HALF, 128), 0)
    lanes_in = lax.broadcasted_iota(jnp.int32, (HALF, 128), 1)
    part_y = [at((yh + o) % 2, 0, 0, 0) for o in (0, 1)]
    part_x = [at(0, (x + o) % XS, 0, 0) for o in range(XS)]
    part_z = [at(0, 0, (z + o) % ZS, 0) for o in range(ZS)]
    part_core = [(core + o) % 2 for o in (0, 1)]

    def compute(e, tile):
        base, rows = TILES[tile]
        first = e * OWN + base
        for u in range(rows // HALF):
            side, path, dx, dz = SOURCES[base // HALF + u]
            block = part_y[side] + part_x[dx % XS] + part_z[dz % ZS] + part_core[e]
            here = slice(u * HALF, (u + 1) * HALF)
            oh[here, :] = jnp.where(lanes_in == block, 1.0, 0.0).astype(BF)
            pos[here, :] = rows_in + (block * TOK + path * HALF)

        keys = kv[pl.ds(first, rows), 0:256]
        blocks = oh[0:rows, :]
        scores = [
            dot(
                jnp.concatenate([keys[:, kh * HEAD : (kh + 1) * HEAD], blocks], axis=1), qx[kh]
            )
            for kh in range(KV)
        ]
        vals_t = kv[pl.ds(first, rows), 256:512].T

        def code(rot, axis):
            return jnp.concatenate(
                [
                    jnp.clip(
                        jnp.floor(lax.slice_in_dim(rot, j * HEAD, (j + 1) * HEAD, axis=axis) * forward[j] + 0.5),
                        -level[j],
                        level[j],
                    ).astype(BF)
                    for j in range(KV)
                ],
                axis=axis,
            )

        coded_k = code(dot(keys, h2[...]), 1)
        coded_v = code(dot(h2[...], vals_t), 0)
        two = dot(coded_k, qd[...])
        for kh in range(KV):
            sc = scores[kh]
            old = m_p[kh]
            top = jnp.maximum(old, jnp.max(sc, axis=0, keepdims=True))
            w = jnp.exp2(sc * SCORE - top * SCORE)
            fade = jnp.exp2((old - top) * SCORE)
            m_p[kh] = top
            l_p[kh] = l_p[kh] * fade + jnp.sum(w, axis=0, keepdims=True)
            o_p[kh] = o_p[kh] * fade + dot(vals_t[kh * HEAD : (kh + 1) * HEAD, :], w.astype(BF))
        sc = jnp.where(pos[0:rows, :] < limits, two[:, 0:128] + two[:, 128:256], VERY_LOW)
        old = m_d[...]
        top = jnp.maximum(old, jnp.max(sc, axis=0, keepdims=True))
        w = jnp.exp2(sc * SCORE - top * SCORE)
        fade = jnp.exp2((old - top) * SCORE)
        m_d[...] = top
        l_d[...] = l_d[...] * fade + jnp.sum(w, axis=0, keepdims=True)
        o_d[...] = o_d[...] * fade + dot(coded_v, w.astype(BF))


    shared = 0
    for k, (_, tiles) in enumerate(PLAN):
        if k > 1:
            wave_copy(k).wait_recv()
            forwards(k)
            to_sibling(k).start()
        for e, t in tiles:
            while e == 1 and shared <= NEED[t]:
                to_sibling(shared).wait_recv()
                shared += 1
            compute(e, t)

    turned = jnp.where(first_head, o_d[0:128, :], o_d[128:256, :])
    high = turned.astype(BF)
    low = (turned - high.astype(F32)).astype(BF)
    sign = h2[0:128, 0:128]
    plain = (dot(sign, high) + dot(sign, low)) * jnp.where(first_head, backward[0], backward[1])
    plain = plain + o_0[...] * jnp.exp2((m_0[...] - m_d[...]) * SCORE)
    dattn[...] = (plain / l_d[...]).T
    total = jnp.zeros((8, 128), F32)
    for h in range(KV * GROUP):
        a = dattn[h * 8 : (h + 1) * 8, :]
        total = total + a * a
    sq_mine[TOK : TOK + 8, :] = jnp.broadcast_to(jnp.sum(total, axis=1, keepdims=True), (8, 128))

    total = jnp.zeros((TOK, 128), F32)
    for kh in range(KV):
        done = (o_p[kh] / l_p[kh]).T
        attn[kh] = done
        for g in range(GROUP):
            a = done[g * TOK : (g + 1) * TOK, :]
            total = total + a * a
    sq_mine[0:TOK, :] = jnp.broadcast_to(jnp.sum(total, axis=1, keepdims=True), (TOK, 128))
    swap = pltpu.make_async_remote_copy(
        src_ref=sq_mine,
        dst_ref=sq_theirs,
        send_sem=g_send,
        recv_sem=g_recv,
        device_id=(s, 1 - grp),
        device_id_type=MESH,
    )
    swap.start()

    for c in ycopies:
        c.wait_send()
    for k in range(NW):
        if ORDER[k][0] > 0:
            wave_copy(k).wait_send()
        to_sibling(k).wait_send()
    swap.wait()
    norm = lax.rsqrt((sq_mine[...] + sq_theirs[...]) / WIDE + EPS)
    for kh in range(KV):
        for g in range(GROUP):
            h = kh * GROUP + g
            out_ref[:, h * HEAD : (h + 1) * HEAD] = (
                attn[kh, g * TOK : (g + 1) * TOK, :] * norm[0:TOK]
            ).astype(BF)
            a = (dattn[h * 8 : (h + 1) * 8, :] * norm[TOK : TOK + 8]).astype(BF)
            for t in range(STEPS):
                dout_ref[t, :, h * HEAD : (h + 1) * HEAD] = a[t * ROWS : (t + 1) * ROWS, :]


def local(q, k, v, mask, widths, exps, dq, nk, nv, ctx):
    vmem = pl.BlockSpec(memory_space=pltpu.VMEM)
    hbm = pl.BlockSpec(memory_space=pltpu.HBM)
    dma = pltpu.SemaphoreType.DMA
    return pl.pallas_call(
        kernel,
        out_shape=(
            jax.ShapeDtypeStruct(q.shape, BF),
            jax.ShapeDtypeStruct(dq.shape, BF),
        ),
        in_specs=[hbm] * 10,
        out_specs=(vmem, vmem),
        scratch_shapes=[
            pltpu.SMEM((KV,), jnp.int32),
            pltpu.SMEM((KV,), jnp.int32),
            pltpu.SMEM((ROWS,), jnp.int32),
            pltpu.VMEM(q.shape, BF),
            pltpu.VMEM(mask.shape, jnp.int32),
            pltpu.VMEM(dq.shape, BF),
            pltpu.VMEM(nk.shape, BF),
            pltpu.VMEM(nv.shape, BF),
            pltpu.VMEM((2 * OWN, 512), BF),
            pltpu.VMEM((KV, 256, 512), BF),
            pltpu.VMEM((256, 256), BF),
            pltpu.VMEM((256, 256), BF),
            pltpu.VMEM((TILE, 128), BF),
            pltpu.VMEM((TILE, 128), jnp.int32),
            pltpu.VMEM((KV, 1, 512), F32),
            pltpu.VMEM((KV, 1, 512), F32),
            pltpu.VMEM((KV, 128, 512), F32),
            pltpu.VMEM((1, 128), F32),
            pltpu.VMEM((1, 128), F32),
            pltpu.VMEM((256, 128), F32),
            pltpu.VMEM((1, 128), F32),
            pltpu.VMEM((128, 128), F32),
            pltpu.VMEM((128, 128), F32),
            pltpu.VMEM((128, 256), F32),
            pltpu.VMEM((128, 256), F32),
            pltpu.VMEM((KV, 512, 128), F32),
            pltpu.VMEM((128, 128), F32),
            pltpu.VMEM((TOK + 8, 128), F32),
            pltpu.VMEM((TOK + 8, 128), F32),
            dma((10,)),
            dma((2,)),
            dma((NW,)),
            dma((NW,)),
            dma((NW,)),
            dma((NW,)),
            dma,
            dma,
        ],
        compiler_params=pltpu.CompilerParams(
            collective_id=0, has_side_effects=True, vmem_limit_bytes=67_043_328
        ),
    )(q, k, v, mask, widths, exps, dq, nk, nv, ctx)


def solution(mesh):
    placed = (
        P("seq", "grp"),
        P("seq", "grp"),
        P("seq", "grp"),
        P(),
        P("grp"),
        P("grp"),
        P(None, "seq", "grp"),
        P(None, "seq", "grp"),
        P(None, "seq", "grp"),
        P("seq"),
    )
    return jax.shard_map(
        local,
        mesh=mesh,
        in_specs=placed,
        out_specs=(P("seq", "grp"), P(None, "seq", "grp")),
        check_vma=False,
    )
```
